128 devices in a mesh: dp: 32 (over z, x_lo, y), mp: 4 (over x_hi, core).
Axes of the slice: x: 4 (x_hi: 2, x_lo: 2; x = x_hi * 2 + x_lo), y: 4, z: 4, core: 2. Of those that a mesh axis runs over, the one named last changes fastest.
Arguments:
- series: bfloat16 [32768, 1280], P('dp'), may hold values from -6 to 6
- inner_weight: bfloat16 [1280, 1280], P('mp'), may hold values from -0.15625 to 0.15625
- inner_bias: float32 [1280], P('mp'), may hold values from -3 to 3
- outer_weight: bfloat16 [1280, 1280], P('mp'), may hold values from -0.15625 to 0.15625
- skip_weight: bfloat16 [1280, 1280], P('mp'), may hold values from -0.15625 to 0.15625
- outer_bias: float32 [1280], replicated, may hold values from -3 to 3
- targets: float32 [32768, 128], P('dp'), may hold values from -9 to 9
- levels: int32 [10], replicated, may hold values from 0 to 8
- counts: int32 [2048], P('dp'), may hold values from 1 to 16
Outputs:
- input_grad: float32 [32768, 1280], P('dp', 'mp')
- inner_grad: float32 [1280, 1280], P(('mp', 'dp'))
- outer_grad: float32 [1280, 1280], P(('mp', 'dp'))
- skip_grad: float32 [1280, 1280], P(('mp', 'dp'))
- inbias_grad: float32 [1280], P(('mp', 'dp'))
- outbias_grad: float32 [1280], P('dp')
The draws below stay inside these ranges and needn't reach their ends.
All inputs are finite; a program needn't handle non-finite values.
Results may differ from the reference program's by a relative error of at most 0.0039.
Values may be sent and summed in bfloat16 or wider, within the bound.
A program may use at most 64 MiB of HBM per device.

```python
import jax
import jax.numpy as jnp
from jax import lax

D = 1280
H = 1280
P_SIZE = 128
Q = 10
LEVELS = 9
PATCHES = 16
OUT = 1280
WINDOWS = 2048
ROWS = 32768


def place_ends(drawn, key, low, high):
    place = [jax.random.randint(jax.random.fold_in(key, axis), (), 0, length) for axis, length in enumerate(drawn.shape)]
    widest = drawn.shape.index(max(drawn.shape))
    beside = place[:widest] + [(place[widest] + 1) % drawn.shape[widest]] + place[widest + 1:]
    return drawn.at[tuple(place)].set(low).at[tuple(beside)].set(high)


def steps_of(stream_key, shape, shards, least, high):
    def one(position, shards_of):
        steps = jax.random.uniform(jax.random.fold_in(jax.random.fold_in(stream_key, 6), position), (shards_of,), jnp.float32, least / len(shards), high / len(shards))
        return jnp.repeat(jnp.exp(steps), shape[position] // shards_of).reshape((-1,) + (1,) * (len(shape) - position - 1))

    factor_of = one(*shards[0])
    for cut in shards[1:]:
        factor_of = factor_of * one(*cut)
    return factor_of


def normal_values(key, extent, width, limit, split=(), kind=jnp.bfloat16):
    drawn = width * jax.random.normal(key, extent, jnp.float32)
    if split:
        drawn = drawn * steps_of(key, extent, split, -0.22, 0.18)
    return jnp.clip(drawn, -limit, limit).astype(kind)


def setup_inputs(seed: int = 0) -> dict:
    key_list = jax.random.split(jax.random.key(seed), 10)
    series = normal_values(key_list[0], (ROWS, D), 1.0, 6.0, ((0, 32),))
    inner_weight = normal_values(key_list[1], (H, D), D ** -0.5, 0.15625, ((0, 4),))
    inner_bias = normal_values(key_list[2], (H,), 1.0, 3.0, ((0, 4),), jnp.float32)
    outer_weight = normal_values(key_list[3], (H, OUT), H ** -0.5, 0.15625, ((0, 4),))
    skip_weight = normal_values(key_list[4], (D, OUT), D ** -0.5, 0.15625, ((0, 4),))
    outer_bias = normal_values(key_list[5], (OUT,), 0.7, 3.0, (), jnp.float32)
    targets = normal_values(key_list[6], (ROWS, P_SIZE), 1.5, 9.0, ((0, 32),), jnp.float32)
    levels = place_ends(jax.random.randint(key_list[7], (Q,), 0, LEVELS), jax.random.fold_in(key_list[7], 1), 0, LEVELS - 1).astype(jnp.int32)
    counts = place_ends(jax.random.randint(key_list[8], (WINDOWS,), 1, PATCHES + 1), jax.random.fold_in(key_list[8], 1), 1, PATCHES).astype(jnp.int32)
    return {"series": series, "inner_weight": inner_weight, "inner_bias": inner_bias, "outer_weight": outer_weight, "skip_weight": skip_weight, "outer_bias": outer_bias, "targets": targets, "levels": levels, "counts": counts}


huber_width = 0.5


def output_slope(predicted, target_rows, count_rows, levels):
    row_count = predicted.shape[0]
    window_count = count_rows.shape[0]
    patch_count = row_count // window_count
    horizon = target_rows.shape[1]
    quantiles = levels.shape[0]
    fraction = (levels.astype(jnp.float32) + 1.0) / (LEVELS + 1)
    level_cols = jnp.broadcast_to(fraction[None, :], (horizon, quantiles)).reshape(horizon * quantiles)
    spread = jnp.broadcast_to(target_rows[:, :, None], (row_count, horizon, quantiles)).reshape(row_count, horizon * quantiles)
    residue = spread - predicted
    slopes = jnp.where(residue >= 0, level_cols, 1.0 - level_cols) * jnp.clip(residue / huber_width, -1.0, 1.0)
    positions = lax.broadcasted_iota(jnp.int32, (window_count, patch_count), 1)
    validity = (positions < count_rows[:, None]).astype(jnp.float32)
    weights = (validity / count_rows[:, None].astype(jnp.float32)).reshape(row_count, 1)
    return (-slopes * weights).astype(jnp.bfloat16)


def reference(series, inner_weight, inner_bias, outer_weight, skip_weight, outer_bias, targets, levels, counts):
    preact = jnp.dot(series, inner_weight.T, preferred_element_type=jnp.float32) + inner_bias
    sigmoids = jax.nn.sigmoid(preact)
    hidden = (preact * sigmoids).astype(jnp.bfloat16)
    predicted = jnp.dot(hidden, outer_weight, preferred_element_type=jnp.float32) + jnp.dot(series, skip_weight, preferred_element_type=jnp.float32) + outer_bias
    out_grad = output_slope(predicted, targets, counts, levels)
    backflow = jnp.dot(out_grad, outer_weight.T, preferred_element_type=jnp.float32)
    hidden_grad = (backflow * sigmoids * (1.0 + preact * (1.0 - sigmoids))).astype(jnp.bfloat16)
    input_grad = jnp.dot(hidden_grad, inner_weight, preferred_element_type=jnp.float32) + jnp.dot(out_grad, skip_weight.T, preferred_element_type=jnp.float32)
    rescale = 1.0 / WINDOWS
    inner_grad = jnp.dot(hidden_grad.T, series, preferred_element_type=jnp.float32) * rescale
    outer_grad = jnp.dot(hidden.T, out_grad, preferred_element_type=jnp.float32) * rescale
    skip_grad = jnp.dot(series.T, out_grad, preferred_element_type=jnp.float32) * rescale
    inbias_grad = jnp.sum(hidden_grad.astype(jnp.float32), axis=0) * rescale
    outbias_grad = jnp.sum(out_grad.astype(jnp.float32), axis=0) * rescale
    return (input_grad, inner_grad, outer_grad, skip_grad, inbias_grad, outbias_grad)
```

```python
import jax
import jax.numpy as jnp
from jax import lax
from jax.experimental import pallas as pl
from jax.experimental.pallas import tpu as pltpu
from jax.sharding import PartitionSpec as P

MESH = pl.DeviceIdType.MESH
F32 = jnp.float32
BF16 = jnp.bfloat16
LEVELS = 9
PATCHES = 16
QUANTILES = 10
HUBER_WIDTH = 0.5

D = 1280
SHARD = 320
PAD = 384
HALF = 2 * PAD
CHIP = 512
CORE = 256
OWN = 640
C1, C2, C3 = 160, 40, 10
LANES = 640

NN = (((1,), (0,)), ((), ()))
NT = (((1,), (1,)), ((), ()))


def mm(a, b, dims=NN):
    return lax.dot_general(a, b, dims, preferred_element_type=F32)


def rem(a, n):
    return lax.rem(a, jnp.int32(n))


def div(a, n):
    return lax.div(a, jnp.int32(n))


def part(index, size):
    return pl.ds(pl.multiple_of(index * size, size), size)


ORDERS = ("xyz", "yzx", "zxy")


def split(n, size):
    q = (
        (n >= size).astype(jnp.int32)
        + (n >= 2 * size).astype(jnp.int32)
        + (n >= 3 * size).astype(jnp.int32)
    )
    return q, n - q * size


def natural(n, order):
    d1, n = split(n, C1)
    d2, n = split(n, C2)
    d3, r = split(n, C3)
    at = dict(zip(order, (d1, d2, d3)))
    x_hi = (at["x"] >= 2).astype(jnp.int32)
    x_lo = at["x"] - 2 * x_hi
    return x_hi * PAD + (at["z"] * 8 + x_lo * 4 + at["y"]) * 10 + r


def kernel(
    series_hbm, wi_hbm, wo_hbm, ws_hbm, ib_hbm, ob_hbm, targets_hbm, levels_ref, counts_ref,
    in_out, gi_out, go_out, gs_out, ib_out, ob_out,
    S, Wi, Wo, Ws, IB, OB, T, sel, perm, isel, isel_send, sH, H, DV, LT, HG, OG,
    spread, tau, p_send, p_recv, p_own, G, ST, RA, RD, RSUM, T2, acc1, ST2, R2, acc2, F3, ST3, R3,
    bsend, brecv, igf, ig_send, ig_recv, outs,
    lsem, ssem, rsem,
):
    dp = lax.axis_index("dp")
    mp = lax.axis_index("mp")
    core = rem(mp, 2)
    x_hi = div(mp, 2)
    z = div(dp, 8)
    x_lo = rem(div(dp, 4), 2)
    y = rem(dp, 4)
    x = x_hi * 2 + x_lo
    other_hi = 1 - x_hi

    def device(x, y, z, core):
        return {"dp": z * 8 + rem(x, 2) * 4 + y, "mp": div(x, 2) * 2 + core}

    pos = {"x": x, "y": y, "z": z}

    def along(axis, k):
        at = dict(pos)
        at[axis] = rem(at[axis] + k, 4)
        return device(at["x"], at["y"], at["z"], core)

    partner = device(x, y, z, 1 - core)
    cross = device(3 - x, y, z, core)
    beside = device(x + 1 - 2 * x_lo, y, z, core)

    loads = []

    def load(src, dst):
        c = pltpu.make_async_copy(src, dst, lsem.at[len(loads)])
        c.start()
        loads.append(c)
        return c

    own_rows = pl.ds(pl.multiple_of(x_hi * PAD, 128), SHARD)
    l_i = load(wi_hbm, Wi.at[own_rows, :])
    l_s = load(ws_hbm, Ws.at[own_rows, :])
    l_o = load(wo_hbm, Wo.at[own_rows, :])
    l_ib = load(ib_hbm, IB.at[x_hi])
    l_series = load(series_hbm.at[part(x_hi, CHIP), :], S)
    l_t = load(targets_hbm.at[part(x_hi * 2 + core, CORE), :], T)
    l_ob = load(ob_hbm, OB)

    barrier = pltpu.get_barrier_semaphore()
    peers = [partner] + [along(a, k) for a in "xyz" for k in (1, 2, 3)]
    for peer in peers:
        pl.semaphore_signal(barrier, inc=1, device_id=peer, device_id_type=MESH)
    pl.semaphore_wait(barrier, len(peers))

    sent = []

    def send(src, dst, to):
        i = len(sent)
        c = pltpu.make_async_remote_copy(
            src_ref=src, dst_ref=dst, send_sem=ssem.at[i], recv_sem=rsem.at[i],
            device_id=to, device_id_type=MESH,
        )
        c.start()
        sent.append(c)
        return c

    weights = (Wi, Ws, Wo)
    axis_of = (y, z)

    def quarter(w, hi, color, q, lanes=None):
        start, size = lanes or (0, LANES)
        return weights[w].at[
            pl.ds(pl.multiple_of(hi * PAD + q * 80, 16), 80),
            pl.ds(pl.multiple_of(color * LANES + start, 128), size),
        ]

    def on_color(color, a, b):
        return jnp.where(color == 0, a, b)

    first, second = x_lo, 1 - x_lo

    def ring(color):
        up = {k: on_color(color, along("y", 1)[k], along("z", 1)[k]) for k in ("dp", "mp")}
        down = {k: on_color(color, along("y", 3)[k], along("z", 3)[k]) for k in ("dp", "mp")}
        return on_color(color, y, z), up, down

    for l in (l_i, l_s, l_o, l_ib):
        l.wait()
    crossed = []
    for w in range(3):
        q = on_color(second, y, z)
        piece = quarter(w, x_hi, second, q)
        crossed.append(send(piece, piece, cross))
    b_crossed = send(IB.at[x_hi], IB.at[x_hi], cross)

    for W in weights:
        for j in range(2):
            W[pl.ds(j * PAD + SHARD, PAD - SHARD), :] = jnp.zeros((PAD - SHARD, D), BF16)

    def one_hot_sel(k):
        def body(i, _):
            h = lax.broadcasted_iota(jnp.int32, (128, D), 0) + i * 128
            col = lax.broadcasted_iota(jnp.int32, (128, D), 1)
            hi = (h >= PAD).astype(jnp.int32)
            j = h - hi * PAD
            want = hi * 640 + k * SHARD + j
            sel[part(i, 128), :] = jnp.where((col == want) & (j < SHARD), 1.0, 0.0).astype(BF16)
            return 0

        lax.fori_loop(0, HALF // 128, body, 0)

    def first_forward(w):
        q, up, down = ring(first)
        crossed[w].wait_recv()
        piece = quarter(w, other_hi, first, q)
        return send(piece, piece, beside), send(piece, piece, up), send(piece, piece, down)

    def second_forward(w, c):
        q, up, down = ring(second)
        c.wait_recv()
        piece = quarter(w, other_hi, second, q)
        return send(piece, piece, up), send(piece, piece, down)

    def relay(w, color, from_below, from_above):
        q, up, down = ring(color)
        cut = PAD if w % 2 == 0 else 256
        from_below.wait_recv()
        a = quarter(w, other_hi, color, rem(q + 3, 4), (0, cut))
        s1 = send(a, a, up)
        from_above.wait_recv()
        b = quarter(w, other_hi, color, rem(q + 1, 4), (cut, LANES - cut))
        return s1, send(b, b, down)

    one_hot_sel(core)
    l_series.wait()

    def sel_body(i, _):
        sH[:, part(i, 256)] = mm(S[...], sel[part(i, 256), :], NT).astype(BF16)
        return 0

    f0 = first_forward(0)
    lax.fori_loop(0, 3, sel_body, 0)
    f1 = first_forward(1)

    for k in range(3):
        def perm_body(i, _, k=k):
            n = lax.broadcasted_iota(jnp.int32, (128, 128), 0) + i * 128
            want = natural(n, ORDERS[k])
            lane = lax.broadcasted_iota(jnp.int32, (128, 128), 1)
            for t in range(HALF // 128):
                perm[k, part(i, 128), pl.ds(t * 128, 128)] = jnp.where(
                    lane + t * 128 == want, 1.0, 0.0
                ).astype(BF16)
            return 0

        lax.fori_loop(0, OWN // 128, perm_body, 0)
        if k == 0:
            s0 = second_forward(0, f0[0])
            r0 = relay(0, first, f0[1], f0[2])
            f2 = first_forward(2)

    def transposed(k, src):
        def body(i, _):
            LT[k, :, part(i, 256)] = mm(perm[k], src[part(i, 256), :], NT).astype(BF16)
            return 0

        lax.fori_loop(0, CHIP // 256, body, 0)

    s1 = second_forward(1, f1[0])
    r1 = relay(1, first, f1[1], f1[2])
    transposed(0, sH)
    s2 = second_forward(2, f2[0])
    r0b = relay(0, second, s0[0], s0[1])

    l_t.wait()
    l_ob.wait()
    col = lax.broadcasted_iota(jnp.int32, (128, D), 1)
    row = lax.broadcasted_iota(jnp.int32, (128, D), 0)
    off = col - row * QUANTILES
    spreader = jnp.where((off >= 0) & (off < QUANTILES), 1.0, 0.0).astype(F32)
    spread[...] = (
        lax.dot_general(
            T[...], spreader, NN, precision=lax.Precision.HIGHEST, preferred_element_type=F32
        )
        - OB[...]
    )
    levels_rows = jnp.zeros((128, D), F32)
    for c in range(QUANTILES):
        level = (jnp.full((128, D), levels_ref[c], jnp.int32).astype(F32) + 1.0) / (LEVELS + 1)
        levels_rows = levels_rows + jnp.where(off == c, level, 0.0)
    tau[...] = jnp.sum(levels_rows, axis=0, keepdims=True)

    r2 = relay(2, first, f2[1], f2[2])
    r1b = relay(1, second, s1[0], s1[1])
    for c in r0 + r0b:
        c.wait_recv()
    b_crossed.wait_recv()

    def hidden_body(i, _):
        cols = part(i, 128)
        bias = IB[div(i, 3), :, part(rem(i, 3), 128)]
        pre = mm(S[...], Wi[part(i, 128), :], NT) + bias
        sig = jax.nn.sigmoid(pre)
        H[:, cols] = (pre * sig).astype(BF16)
        DV[:, cols] = sig * (1.0 + pre * (1.0 - sig))
        return 0

    lax.fori_loop(0, HALF // 128, hidden_body, 0)
    r2b = relay(2, second, s2[0], s2[1])
    transposed(1, H)
    for c in r1 + r1b + r2 + r2b:
        c.wait_recv()

    def predict(rows, dst):
        def body(i, _):
            cols = part(i, 256)
            dst[:, cols] = mm(H[rows, :], Wo[:, cols]) + mm(sH[rows, :], Ws[:, cols])
            return 0

        lax.fori_loop(0, D // 256, body, 0)

    mine, theirs = part(core, CORE), part(1 - core, CORE)
    predict(theirs, p_send)
    p_copy = send(p_send, p_recv, partner)
    predict(mine, p_own)
    p_copy.wait_recv()

    def slope_body(w, _):
        rows = part(w, PATCHES)
        count = counts_ref[(x_hi * 2 + core) * (CORE // PATCHES) + w]
        counted = jnp.full((PATCHES, 128), count, jnp.int32)
        valid = lax.broadcasted_iota(jnp.int32, (PATCHES, 128), 0) < counted
        weight = (jnp.where(valid, 1.0, 0.0) / counted.astype(F32))[:, :1]
        residue = spread[rows, :] - (p_own[rows, :] + p_recv[rows, :])
        t = tau[...]
        slopes = jnp.where(residue >= 0, t, 1.0 - t) * jnp.clip(residue / HUBER_WIDTH, -1.0, 1.0)
        OG[pl.ds(pl.multiple_of(core * CORE + w * PATCHES, PATCHES), PATCHES), :] = (
            -slopes * weight
        ).astype(BF16)
        return 0

    lax.fori_loop(0, CORE // PATCHES, slope_body, 0)
    og_copy = send(OG.at[mine, :], OG.at[mine, :], partner)

    def isel_body(dst):
        def body(i, _):
            dst[:, part(i, 256)] = mm(Wi[...], sel[part(i, 256), :], NT).astype(BF16)
            return 0

        lax.fori_loop(0, HALF // 256, body, 0)

    og_copy.wait_recv()

    def halves(h):
        return pl.ds(h * LANES, LANES)

    def chunk(p, k):
        return part(rem(p + k, 4), C1)

    def gradient(k, right):
        def body(i, _):
            cols = part(i, 256)
            g = mm(LT[k], right[:, cols])
            G[k, :, cols] = g
            ST[k, :, cols] = g.astype(BF16)
            return 0

        lax.fori_loop(0, D // 256, body, 0)
        axis = ORDERS[k][0]
        p = pos[axis]
        up, down = along(axis, 1), along(axis, 3)
        return (
            send(ST.at[k, chunk(p, 2), halves(0)], RA.at[k, 0], up),
            send(ST.at[k, chunk(p, 2), halves(1)], RA.at[k, 1], down),
            send(ST.at[k, chunk(p, 1), halves(1)], RD.at[k, 0], up),
            send(ST.at[k, chunk(p, 3), halves(0)], RD.at[k, 1], down),
        )

    def pass_on(k, step):
        axis = ORDERS[k][0]
        p = pos[axis]
        out = []
        for h, hop in ((0, 1), (1, 3)):
            step[h].wait_recv()

            def body(i, _, h=h, hop=hop):
                rows = pl.ds(pl.multiple_of(rem(p + hop, 4) * C1 + i * 32, 32), 32)
                T2[k, h, part(i, 32), :] = (
                    G[k, rows, halves(h)] + RA[k, h, part(i, 32), :].astype(F32)
                ).astype(BF16)
                return 0

            lax.fori_loop(0, C1 // 32, body, 0)
            out.append(send(T2.at[k, h], RSUM.at[k, h], along(axis, hop)))
        return out

    def second_phase(k, step, passed):
        p = pos[ORDERS[k][0]]
        for c in (step[2], step[3], passed[0], passed[1]):
            c.wait_recv()

        def body(i, _):
            here = part(i, 32)
            rows = pl.ds(pl.multiple_of(p * C1 + i * 32, 32), 32)
            for h in range(2):
                acc1[k, here, halves(h)] = (
                    G[k, rows, halves(h)]
                    + RSUM[k, h, here, :].astype(F32)
                    + RD[k, 1 - h, here, :].astype(F32)
                )
            return 0

        lax.fori_loop(0, C1 // 32, body, 0)
        for q in range(4):
            ST2[k, q] = acc1[k, pl.ds(q * C2, C2), :].astype(BF16)
        axis = ORDERS[k][1]
        p2 = pos[axis]
        return [send(ST2.at[k, rem(p2 + o, 4)], R2.at[k, o - 1], along(axis, o)) for o in (1, 3, 2)]

    def third_phase(k, step):
        axis = ORDERS[k][1]
        p2 = pos[axis]
        for c in step:
            c.wait_recv()
        total = acc1[k, pl.ds(pl.multiple_of(p2 * C2, 8), C2), :]
        for o in range(3):
            total = total + R2[k, o].astype(F32)
        acc2[k] = total
        for q in range(4):
            piece = acc2[k, pl.ds(q * C3, C3), :]
            F3[k, q] = piece
            ST3[k, q] = piece.astype(BF16)
        axis = ORDERS[k][2]
        p3 = pos[axis]
        return [send(ST3.at[k, rem(p3 + o, 4)], R3.at[k, o - 1], along(axis, o)) for o in (1, 3, 2)]

    rescale = 1.0 / 2048

    def finish(k, step, out):
        p3 = pos[ORDERS[k][2]]
        for c in step:
            c.wait_recv()
        total = F3[k, p3]
        for o in range(3):
            total = total + R3[k, o].astype(F32)
        out[...] = total * rescale

    skip1 = gradient(0, OG)
    outer1 = gradient(1, OG)

    def backflow_body(i, _):
        cols = part(i, 256)
        back = mm(OG[...], Wo[cols, :], NT)
        HG[core, :, cols] = (back * DV[:, cols]).astype(BF16)
        return 0

    lax.fori_loop(0, HALF // 256, backflow_body, 0)
    hg_copy = send(HG.at[core], HG.at[core], partner)
    transposed(2, HG.at[core])
    inner1 = gradient(2, S)

    bsend[0, :, pl.ds(0, HALF)] = jnp.sum(HG[core].astype(F32), axis=0, keepdims=True)
    bsend[0, :, pl.ds(HALF, D)] = jnp.sum(OG[...].astype(F32), axis=0, keepdims=True)

    def bias_send(i):
        axis = "xyz"[i]
        return [send(bsend.at[i], brecv.at[i, o - 1], along(axis, o)) for o in (1, 2, 3)]

    def bias_add(i, copies):
        for c in copies:
            c.wait_recv()
        bsend[i + 1] = bsend[i] + brecv[i, 0] + brecv[i, 1] + brecv[i, 2]

    bias1 = bias_send(0)
    isel_body(isel.at[core])
    skip2 = pass_on(0, skip1)
    one_hot_sel(1 - core)
    isel_body(isel_send)
    isel_copy = send(isel_send, isel.at[core], partner)
    outer2 = pass_on(1, outer1)
    bias_add(0, bias1)
    bias2 = bias_send(1)
    inner2 = pass_on(2, inner1)

    hg_copy.wait_recv()
    isel_copy.wait_recv()

    def input_body(i, _):
        cols = part(i, 256)
        igf[:, cols] = (
            mm(HG[0], isel[0, :, cols])
            + mm(HG[1], isel[1, :, cols])
            + mm(OG[...], Ws[cols, :], NT)
        )
        return 0

    lax.fori_loop(0, HALF // 256, input_body, 0)
    ig_send[...] = igf[:, part(other_hi, PAD)].astype(BF16)
    ig_copy = send(ig_send, ig_recv, along("x", 2))
    outs[0] = igf[:, part(x_hi, PAD)][:, :SHARD]
    out0 = pltpu.make_async_copy(outs.at[0], in_out.at[part(x_hi, CHIP), :], lsem.at[len(loads)])
    out0.start()

    skip3 = second_phase(0, skip1, skip2)
    outer3 = second_phase(1, outer1, outer2)
    bias_add(1, bias2)
    bias3 = bias_send(2)
    inner3 = second_phase(2, inner1, inner2)
    skip4 = third_phase(0, skip3)
    outer4 = third_phase(1, outer3)
    ig_copy.wait_recv()
    outs[1] = ig_recv[:, :SHARD].astype(F32)
    out1 = pltpu.make_async_copy(
        outs.at[1], in_out.at[part(other_hi, CHIP), :], lsem.at[len(loads) + 1]
    )
    out1.start()
    inner4 = third_phase(2, inner3)
    bias_add(2, bias3)

    def pick(v, start):
        n = v.shape[1]
        i = lax.broadcasted_iota(jnp.int32, (n, 128), 0)
        j = lax.broadcasted_iota(jnp.int32, (n, 128), 1)
        hot = jnp.where(i == j + start, 1.0, 0.0).astype(F32)
        return lax.dot_general(
            jnp.broadcast_to(v, (8, n)), hot, NN,
            precision=lax.Precision.HIGHEST, preferred_element_type=F32,
        )[:1] * rescale

    ib_out[...] = pick(bsend[3, :, pl.ds(0, HALF)], x_hi * PAD + dp * 10)[:, :10]
    ob_out[...] = pick(bsend[3, :, pl.ds(HALF, D)], dp * 40)[:, :40]
    finish(0, skip4, gs_out)
    finish(1, outer4, go_out)
    finish(2, inner4, gi_out)
    for c in sent:
        c.wait_send()
    out0.wait()
    out1.wait()


N_SENDS = 96


def on_device(series, wi, ib, wo, ws, ob, targets, levels, counts):
    hbm = pl.BlockSpec(memory_space=pl.ANY)
    vmem = pl.BlockSpec(memory_space=pltpu.VMEM)
    smem = pl.BlockSpec(memory_space=pltpu.SMEM)
    grad = jax.ShapeDtypeStruct((C3, D), F32)
    outs = pl.pallas_call(
        kernel,
        out_shape=(
            jax.ShapeDtypeStruct((2 * CHIP, SHARD), F32), grad, grad, grad,
            jax.ShapeDtypeStruct((1, 10), F32), jax.ShapeDtypeStruct((1, 40), F32),
        ),
        in_specs=[hbm] * 7 + [smem] * 2,
        out_specs=(hbm,) + (vmem,) * 5,
        scratch_shapes=[
            pltpu.VMEM((CHIP, D), BF16),
            pltpu.VMEM((HALF, D), BF16),
            pltpu.VMEM((HALF, D), BF16),
            pltpu.VMEM((HALF, D), BF16),
            pltpu.VMEM((2, 1, PAD), F32),
            pltpu.VMEM((1, D), F32),
            pltpu.VMEM((CORE, 128), F32),
            pltpu.VMEM((HALF, D), BF16),
            pltpu.VMEM((3, OWN, HALF), BF16),
            pltpu.VMEM((2, HALF, HALF), BF16),
            pltpu.VMEM((HALF, HALF), BF16),
            pltpu.VMEM((CHIP, HALF), BF16),
            pltpu.VMEM((CHIP, HALF), BF16),
            pltpu.VMEM((CHIP, HALF), F32),
            pltpu.VMEM((3, OWN, CHIP), BF16),
            pltpu.VMEM((2, CHIP, HALF), BF16),
            pltpu.VMEM((CHIP, D), BF16),
            pltpu.VMEM((CORE, D), F32),
            pltpu.VMEM((1, D), F32),
            pltpu.VMEM((CORE, D), F32),
            pltpu.VMEM((CORE, D), F32),
            pltpu.VMEM((CORE, D), F32),
            pltpu.VMEM((3, OWN, D), F32),
            pltpu.VMEM((3, OWN, D), BF16),
            pltpu.VMEM((3, 2, C1, LANES), BF16),
            pltpu.VMEM((3, 2, C1, LANES), BF16),
            pltpu.VMEM((3, 2, C1, LANES), BF16),
            pltpu.VMEM((3, 2, C1, LANES), BF16),
            pltpu.VMEM((3, C1, D), F32),
            pltpu.VMEM((3, 4, C2, D), BF16),
            pltpu.VMEM((3, 3, C2, D), BF16),
            pltpu.VMEM((3, C2, D), F32),
            pltpu.VMEM((3, 4, C3, D), F32),
            pltpu.VMEM((3, 4, C3, D), BF16),
            pltpu.VMEM((3, 3, C3, D), BF16),
            pltpu.VMEM((4, 1, HALF + D), F32),
            pltpu.VMEM((3, 3, 1, HALF + D), F32),
            pltpu.VMEM((CHIP, HALF), F32),
            pltpu.VMEM((CHIP, PAD), BF16),
            pltpu.VMEM((CHIP, PAD), BF16),
            pltpu.VMEM((2, CHIP, SHARD), F32),
            pltpu.SemaphoreType.DMA((16,)),
            pltpu.SemaphoreType.DMA((N_SENDS,)),
            pltpu.SemaphoreType.DMA((N_SENDS,)),
        ],
        compiler_params=pltpu.CompilerParams(
            collective_id=0, has_side_effects=True, vmem_limit_bytes=62 * 1024 * 1024
        ),
    )(
        series, wi, wo, ws, jnp.pad(ib, (0, PAD - SHARD)).reshape(1, PAD), ob.reshape(1, D),
        targets, levels, counts,
    )
    input_grad, inner, outer, skip, inbias, outbias = outs
    return input_grad, inner, outer, skip, inbias.reshape(10), outbias.reshape(40)


def solution(mesh):
    return jax.shard_map(
        on_device,
        mesh=mesh,
        in_specs=(
            P("dp", None), P("mp", None), P("mp"), P("mp", None), P("mp", None), P(None),
            P("dp", None), P(None), P("dp"),
        ),
        out_specs=(
            P("dp", "mp"), P(("mp", "dp"), None), P(("mp", "dp"), None), P(("mp", "dp"), None),
            P(("mp", "dp")), P("dp"),
        ),
        check_vma=False,
    )
```

```python
import jax
import jax.numpy as jnp
from jax import lax
from jax.experimental import pallas as pl
from jax.experimental.pallas import tpu as pltpu
from jax.sharding import PartitionSpec as P

MESH = pl.DeviceIdType.MESH
F32 = jnp.float32
BF16 = jnp.bfloat16
LEVELS = 9
PATCHES = 16
QUANTILES = 10
HUBER_WIDTH = 0.5

D = 1280
SHARD = 320
PAD = 384
HALF = 2 * PAD
CHIP = 512
CORE = 256
OWN = 640
C1, C2, C3 = 160, 40, 10
LANES = 640

NN = (((1,), (0,)), ((), ()))
NT = (((1,), (1,)), ((), ()))


def mm(a, b, dims=NN):
    return lax.dot_general(a, b, dims, preferred_element_type=F32)


def rem(a, n):
    return lax.rem(a, jnp.int32(n))


def div(a, n):
    return lax.div(a, jnp.int32(n))


def part(index, size):
    return pl.ds(pl.multiple_of(index * size, size), size)


ORDERS = ("xyz", "yzx", "zyx")


def split(n, size):
    q = (
        (n >= size).astype(jnp.int32)
        + (n >= 2 * size).astype(jnp.int32)
        + (n >= 3 * size).astype(jnp.int32)
    )
    return q, n - q * size


def natural(n, order):
    d1, n = split(n, C1)
    d2, n = split(n, C2)
    d3, r = split(n, C3)
    at = dict(zip(order, (d1, d2, d3)))
    x_hi = (at["x"] >= 2).astype(jnp.int32)
    x_lo = at["x"] - 2 * x_hi
    return x_hi * PAD + (at["z"] * 8 + x_lo * 4 + at["y"]) * 10 + r


def kernel(
    series_hbm, wi_hbm, wo_hbm, ws_hbm, ib_ref, ob_ref, targets_hbm, levels_ref, counts_ref,
    in_out, gi_out, go_out, gs_out, ib_out, ob_out,
    S, Wi, Wo, Ws, IB, T, sel, perm, isel, isel_send, sH, H, DV, LT, HG, OG,
    spread, tau, p_send, p_recv, p_own, G, ST, RA, RD, RSUM, T2,
    acc1, ST2, RA2, RD2, RSUM2, T3, acc2, F3, ST3, R3,
    bsend, brecv, igf, ig_send, ig_mid, ig_recv, outs,
    lsem, ssem, rsem,
):
    dp = lax.axis_index("dp")
    mp = lax.axis_index("mp")
    core = rem(mp, 2)
    x_hi = div(mp, 2)
    z = div(dp, 8)
    x_lo = rem(div(dp, 4), 2)
    y = rem(dp, 4)
    x = x_hi * 2 + x_lo
    other_hi = 1 - x_hi

    def device(x, y, z, core):
        return {"dp": z * 8 + rem(x, 2) * 4 + y, "mp": div(x, 2) * 2 + core}

    pos = {"x": x, "y": y, "z": z}

    def along(axis, k):
        at = dict(pos)
        at[axis] = rem(at[axis] + k, 4)
        return device(at["x"], at["y"], at["z"], core)

    partner = device(x, y, z, 1 - core)
    cross = device(3 - x, y, z, core)
    beside = device(x + 1 - 2 * x_lo, y, z, core)

    loads = []

    def load(src, dst):
        c = pltpu.make_async_copy(src, dst, lsem.at[len(loads)])
        c.start()
        loads.append(c)
        return c

    own_rows = pl.ds(pl.multiple_of(x_hi * PAD, 128), SHARD)
    l_i = load(wi_hbm, Wi.at[own_rows, :])
    l_s = load(ws_hbm, Ws.at[own_rows, :])
    l_o = load(wo_hbm, Wo.at[own_rows, :])
    l_series = load(series_hbm.at[part(x_hi, CHIP), :], S)
    l_t = load(targets_hbm.at[part(x_hi * 2 + core, CORE), :], T)

    IB[:, part(x_hi, PAD)] = jnp.concatenate(
        [ib_ref[...].reshape(1, SHARD), jnp.zeros((1, PAD - SHARD), F32)], axis=1
    )
    barrier = pltpu.get_barrier_semaphore()
    peers = [partner] + [along(a, k) for a in "xyz" for k in (1, 2, 3)]
    for peer in peers:
        pl.semaphore_signal(barrier, inc=1, device_id=peer, device_id_type=MESH)
    pl.semaphore_wait(barrier, len(peers))

    sent = []

    def send(src, dst, to):
        i = len(sent)
        c = pltpu.make_async_remote_copy(
            src_ref=src, dst_ref=dst, send_sem=ssem.at[i], recv_sem=rsem.at[i],
            device_id=to, device_id_type=MESH,
        )
        c.start()
        sent.append(c)
        return c

    weights = (Wi, Ws, Wo)
    axis_of = (y, z)

    def quarter(w, hi, color, q, start, size):
        return weights[w].at[
            pl.ds(pl.multiple_of(hi * PAD + q * 80, 16), 80),
            pl.ds(pl.multiple_of(color * LANES + start, 128), size),
        ]

    def on_color(color, a, b):
        return jnp.where(color == 0, a, b)

    first, second = x_lo, 1 - x_lo

    def ring(color):
        up = {k: on_color(color, along("y", 1)[k], along("z", 1)[k]) for k in ("dp", "mp")}
        down = {k: on_color(color, along("y", 3)[k], along("z", 3)[k]) for k in ("dp", "mp")}
        return on_color(color, y, z), up, down

    items = [
        (w, start, size, cut)
        for w in range(3)
        for start, size, cut in ((0, 384, 256 - 128 * (w % 2)), (384, 256, 128))
    ]
    crossed = []
    for i, (w, start, size, _) in enumerate(items):
        if i % 2 == 0:
            (l_i, l_s, l_o)[w].wait()
        piece = quarter(w, x_hi, second, on_color(second, y, z), start, size)
        crossed.append(send(piece, piece, cross))
        if i == 1:
            own_bias = IB.at[:, part(x_hi, PAD)]
            b_crossed = send(own_bias, own_bias, cross)

    for W in weights:
        for j in range(2):
            W[pl.ds(j * PAD + SHARD, PAD - SHARD), :] = jnp.zeros((PAD - SHARD, D), BF16)

    def one_hot_sel(k):
        def body(i, _):
            h = lax.broadcasted_iota(jnp.int32, (128, D), 0) + i * 128
            col = lax.broadcasted_iota(jnp.int32, (128, D), 1)
            hi = (h >= PAD).astype(jnp.int32)
            j = h - hi * PAD
            want = hi * 640 + k * SHARD + j
            sel[part(i, 128), :] = jnp.where((col == want) & (j < SHARD), 1.0, 0.0).astype(BF16)
            return 0

        lax.fori_loop(0, HALF // 128, body, 0)

    beside_of, own_of, relayed = {}, {}, {}

    def forward_first(i):
        w, start, size, _ = items[i]
        q, up, down = ring(first)
        crossed[i].wait_recv()
        piece = quarter(w, other_hi, first, q, start, size)
        beside_of[i] = send(piece, piece, beside)
        own_of[i, 0] = send(piece, piece, up), send(piece, piece, down)

    def forward_second(i):
        w, start, size, _ = items[i]
        q, up, down = ring(second)
        beside_of[i].wait_recv()
        piece = quarter(w, other_hi, second, q, start, size)
        own_of[i, 1] = send(piece, piece, up), send(piece, piece, down)

    def relay(i, turn):
        w, start, size, cut = items[i]
        color = (first, second)[turn]
        q, up, down = ring(color)
        from_below, from_above = own_of[i, turn]
        from_below.wait_recv()
        a = quarter(w, other_hi, color, rem(q + 3, 4), start, cut)
        s1 = send(a, a, up)
        from_above.wait_recv()
        b = quarter(w, other_hi, color, rem(q + 1, 4), start + cut, size - cut)
        relayed[i, turn] = s1, send(b, b, down)

    def arrived(i):
        for turn in range(2):
            for c in relayed[i, turn]:
                c.wait_recv()

    def sel_body(i, _):
        sH[:, part(i, 256)] = mm(S[...], sel[part(i, 256), :], NT).astype(BF16)
        return 0

    def make_perm(k):
        def body(i, _):
            n = lax.broadcasted_iota(jnp.int32, (128, 128), 0) + i * 128
            want = natural(n, ORDERS[k])
            lane = lax.broadcasted_iota(jnp.int32, (128, 128), 1)
            for t in range(HALF // 128):
                perm[k, part(i, 128), pl.ds(t * 128, 128)] = jnp.where(
                    lane + t * 128 == want, 1.0, 0.0
                ).astype(BF16)
            return 0

        lax.fori_loop(0, OWN // 128, body, 0)

    def transposed(k, src):
        def body(i, _):
            LT[k, :, part(i, 256)] = mm(perm[k], src[part(i, 256), :], NT).astype(BF16)
            return 0

        lax.fori_loop(0, CHIP // 256, body, 0)

    def spread_body(i, _):
        cols = part(i, 256)
        col = lax.broadcasted_iota(jnp.int32, (128, 256), 1) + i * 256
        row = lax.broadcasted_iota(jnp.int32, (128, 256), 0)
        off = col - row * QUANTILES
        spreader = jnp.where((off >= 0) & (off < QUANTILES), 1.0, 0.0).astype(F32)
        spread[:, cols] = (
            lax.dot_general(
                T[...], spreader, NN, precision=lax.Precision.HIGHEST, preferred_element_type=F32
            )
            - p_own[:1, cols]
        )
        rows = jnp.zeros((128, 256), F32)
        for c in range(QUANTILES):
            level = jnp.full((128, 256), levels_ref[c], jnp.int32).astype(F32) + 1.0
            rows = rows + jnp.where(off == c, level / (LEVELS + 1), 0.0)
        tau[:, cols] = jnp.sum(rows, axis=0, keepdims=True)
        return 0

    def hidden_body(i, _):
        cols = part(i, 256)
        pre = mm(S[...], Wi[cols, :], NT) + IB[:, cols]
        sig = jax.nn.sigmoid(pre)
        H[:, cols] = (pre * sig).astype(BF16)
        DV[:, cols] = sig * (1.0 + pre * (1.0 - sig))
        return 0

    def isel_body(dst):
        def body(i, _):
            dst[:, part(i, 256)] = mm(sel[...], Wi[part(i, 256), :], NT).astype(BF16)
            return 0

        lax.fori_loop(0, HALF // 256, body, 0)

    one_hot_sel(core)
    l_series.wait()
    p_own[:1, :] = ob_ref[...].reshape(1, D)
    lax.fori_loop(0, 3, sel_body, 0)
    forward_first(0)
    make_perm(0)
    forward_first(1)
    make_perm(1)
    forward_first(2)
    make_perm(2)
    forward_first(3)
    forward_second(0)
    relay(0, 0)
    transposed(0, sH)
    forward_first(4)
    forward_second(1)
    relay(1, 0)
    l_t.wait()
    lax.fori_loop(0, 2, spread_body, 0)
    forward_first(5)
    forward_second(2)
    relay(2, 0)
    lax.fori_loop(2, 5, spread_body, 0)
    forward_second(3)
    relay(3, 0)
    relay(0, 1)
    forward_second(4)
    relay(4, 0)
    relay(1, 1)
    forward_second(5)
    relay(5, 0)
    relay(2, 1)
    arrived(0)
    arrived(1)
    b_crossed.wait_recv()
    relay(3, 1)
    lax.fori_loop(0, 2, hidden_body, 0)
    relay(4, 1)
    lax.fori_loop(2, 3, hidden_body, 0)
    relay(5, 1)
    transposed(1, H)
    isel_body(isel.at[core])
    for i in range(2, 6):
        arrived(i)

    mine, theirs = part(core, CORE), part(1 - core, CORE)

    def predict(rows, cols):
        return mm(H[rows, :], Wo[:, cols]) + mm(sH[rows, :], Ws[:, cols])

    p_copies = []
    for i in range(D // 256):
        cols = pl.ds(i * 256, 256)
        p_send[i] = predict(theirs, cols)
        p_copies.append(send(p_send.at[i], p_recv.at[i], partner))

    def predict_body(i, _):
        cols = part(i, 256)
        p_own[:, cols] = predict(mine, cols)
        return 0

    lax.fori_loop(0, D // 256, predict_body, 0)
    for c in p_copies:
        c.wait_recv()

    def slope_body(w, _):
        rows = part(w, PATCHES)
        count = counts_ref[(x_hi * 2 + core) * (CORE // PATCHES) + w]
        counted = jnp.full((PATCHES, 128), count, jnp.int32)
        valid = lax.broadcasted_iota(jnp.int32, (PATCHES, 128), 0) < counted
        weight = (jnp.where(valid, 1.0, 0.0) / counted.astype(F32))[:, :1]
        for i in range(D // 256):
            cols = pl.ds(i * 256, 256)
            residue = spread[rows, cols] - (p_own[rows, cols] + p_recv[i, rows, :])
            t = tau[:, cols]
            slopes = jnp.where(residue >= 0, t, 1.0 - t) * jnp.clip(
                residue / HUBER_WIDTH, -1.0, 1.0
            )
            OG[pl.ds(pl.multiple_of(core * CORE + w * PATCHES, PATCHES), PATCHES), cols] = (
                -slopes * weight
            ).astype(BF16)
        return 0

    og_copies = []
    for i in range(2):
        lax.fori_loop(8 * i, 8 * i + 8, slope_body, 0)
        rows = OG.at[part(core * 2 + i, 128), :]
        og_copies.append(send(rows, rows, partner))

    def backflow(rows):
        def body(i, _):
            cols = part(i, 256)
            back = mm(OG[rows, :], Wo[cols, :], NT)
            HG[core, rows, cols] = (back * DV[rows, cols]).astype(BF16)
            return 0

        lax.fori_loop(0, HALF // 256, body, 0)

    backflow(mine)
    for c in og_copies:
        c.wait_recv()

    def halves(h):
        return pl.ds(h * LANES, LANES)

    def ring_start(axis, view, ra, rd):
        p = pos[axis]
        up, down = along(axis, 1), along(axis, 3)
        return (
            send(view(rem(p + 2, 4), 0), ra.at[0], up),
            send(view(rem(p + 2, 4), 1), ra.at[1], down),
            send(view(rem(p + 1, 4), 1), rd.at[0], up),
            send(view(rem(p + 3, 4), 0), rd.at[1], down),
        )

    def ring_pass(axis, size, rows, own, ra, out, rsum, step):
        p = pos[axis]
        passed = []
        for h, hop in ((0, 1), (1, 3)):
            step[h].wait_recv()

            def body(i, _, h=h, hop=hop):
                there = pl.ds(pl.multiple_of(rem(p + hop, 4) * size + i * rows, 8), rows)
                here = part(i, rows)
                out[h, here, :] = (
                    own[there, halves(h)] + ra[h, here, :].astype(F32)
                ).astype(BF16)
                return 0

            lax.fori_loop(0, size // rows, body, 0)
            passed.append(send(out.at[h], rsum.at[h], along(axis, hop)))
        return passed

    def ring_end(axis, size, rows, own, rsum, rd, dst, step, passed):
        p = pos[axis]
        for c in (step[2], step[3], passed[0], passed[1]):
            c.wait_recv()

        def body(i, _):
            there = pl.ds(pl.multiple_of(p * size + i * rows, 8), rows)
            here = part(i, rows)
            for h in range(2):
                dst[here, halves(h)] = (
                    own[there, halves(h)]
                    + rsum[h, here, :].astype(F32)
                    + rd[1 - h, here, :].astype(F32)
                )
            return 0

        lax.fori_loop(0, size // rows, body, 0)

    def gradient(k, right):
        def body(i, _):
            cols = part(i, 256)
            g = mm(LT[k], right[:, cols])
            G[k, :, cols] = g
            ST[k, :, cols] = g.astype(BF16)
            return 0

        lax.fori_loop(0, D // 256, body, 0)
        return ring_start(
            ORDERS[k][0], lambda q, h: ST.at[k, part(q, C1), halves(h)], RA.at[k], RD.at[k]
        )

    def pass_on(k, step):
        return ring_pass(
            ORDERS[k][0], C1, 32, G.at[k], RA.at[k], T2.at[k], RSUM.at[k], step
        )

    def second_phase(k, step, passed):
        ring_end(ORDERS[k][0], C1, 32, G.at[k], RSUM.at[k], RD.at[k], acc1.at[k], step, passed)
        for q in range(4):
            ST2[k, q] = acc1[k, pl.ds(q * C2, C2), :].astype(BF16)
        return ring_start(
            ORDERS[k][1], lambda q, h: ST2.at[k, q, :, halves(h)], RA2.at[k], RD2.at[k]
        )

    def pass_on_second(k, step):
        return ring_pass(
            ORDERS[k][1], C2, C2, acc1.at[k], RA2.at[k], T3.at[k], RSUM2.at[k], step
        )

    def third_phase(k, step, passed):
        ring_end(
            ORDERS[k][1], C2, C2, acc1.at[k], RSUM2.at[k], RD2.at[k], acc2.at[k], step, passed
        )
        for q in range(4):
            piece = acc2[k, pl.ds(q * C3, C3), :]
            F3[k, q] = piece
            ST3[k, q] = piece.astype(BF16)
        axis = ORDERS[k][2]
        p3 = pos[axis]
        return [send(ST3.at[k, rem(p3 + o, 4)], R3.at[k, o - 1], along(axis, o)) for o in (1, 3, 2)]

    rescale = 1.0 / 2048

    def finish(k, step, out):
        p3 = pos[ORDERS[k][2]]
        for c in step:
            c.wait_recv()
        total = F3[k, p3]
        for o in range(3):
            total = total + R3[k, o].astype(F32)
        out[...] = total * rescale

    skip1 = gradient(0, OG)
    backflow(theirs)
    hg_copy = send(HG.at[core], HG.at[core], partner)
    transposed(2, HG.at[core])
    inner1 = gradient(2, S)
    outer1 = gradient(1, OG)

    bsend[0, :, pl.ds(0, HALF)] = jnp.sum(HG[core].astype(F32), axis=0, keepdims=True)
    bsend[0, :, pl.ds(HALF, D)] = jnp.sum(OG[...].astype(F32), axis=0, keepdims=True)

    def bias_send(i):
        axis = "xyz"[i]
        return [send(bsend.at[i], brecv.at[i, o - 1], along(axis, o)) for o in (1, 2, 3)]

    def bias_add(i, copies):
        for c in copies:
            c.wait_recv()
        bsend[i + 1] = bsend[i] + brecv[i, 0] + brecv[i, 1] + brecv[i, 2]

    bias1 = bias_send(0)
    one_hot_sel(1 - core)
    skip2 = pass_on(0, skip1)
    isel_body(isel_send)
    isel_copy = send(isel_send, isel.at[core], partner)
    inner2 = pass_on(2, inner1)
    hg_copy.wait_recv()
    isel_copy.wait_recv()

    def input_body(i, _):
        rows = part(i, 256)
        igf[:, rows] = (
            mm(isel[0], HG[0, rows, :], NT)
            + mm(isel[1], HG[1, rows, :], NT)
            + mm(Ws[...], OG[rows, :], NT)
        )
        return 0

    lax.fori_loop(0, CHIP // 256, input_body, 0)
    ig_send[...] = igf[pl.ds(pl.multiple_of(other_hi * PAD, 128), SHARD), :].astype(BF16)
    lower, upper = pl.ds(0, SHARD // 2), pl.ds(SHARD // 2, SHARD // 2)
    ig1 = (
        send(ig_send.at[lower, :], ig_mid.at[lower, :], along("x", 1)),
        send(ig_send.at[upper, :], ig_mid.at[upper, :], along("x", 3)),
    )
    out0 = pltpu.make_async_copy(
        igf.at[own_rows, :], in_out.at[:, part(x_hi, CHIP)], lsem.at[len(loads)]
    )
    out0.start()
    outer2 = pass_on(1, outer1)
    bias_add(0, bias1)
    bias2 = bias_send(1)
    skip3 = second_phase(0, skip1, skip2)
    for c in ig1:
        c.wait_recv()
    ig2 = (
        send(ig_mid.at[lower, :], ig_recv.at[lower, :], along("x", 1)),
        send(ig_mid.at[upper, :], ig_recv.at[upper, :], along("x", 3)),
    )
    inner3 = second_phase(2, inner1, inner2)
    skip4 = pass_on_second(0, skip3)
    outer3 = second_phase(1, outer1, outer2)
    bias_add(1, bias2)
    bias3 = bias_send(2)
    inner4 = pass_on_second(2, inner3)
    skip5 = third_phase(0, skip3, skip4)
    outer4 = pass_on_second(1, outer3)
    for c in ig2:
        c.wait_recv()
    outs[...] = ig_recv[...].astype(F32)
    out1 = pltpu.make_async_copy(
        outs, in_out.at[:, part(other_hi, CHIP)], lsem.at[len(loads) + 1]
    )
    out1.start()
    inner5 = third_phase(2, inner3, inner4)
    outer5 = third_phase(1, outer3, outer4)
    bias_add(2, bias3)

    def pick(v, start):
        n = v.shape[1]
        i = lax.broadcasted_iota(jnp.int32, (n, 128), 0)
        j = lax.broadcasted_iota(jnp.int32, (n, 128), 1)
        hot = jnp.where(i == j + start, 1.0, 0.0).astype(F32)
        return lax.dot_general(
            jnp.broadcast_to(v, (8, n)), hot, NN,
            precision=lax.Precision.HIGHEST, preferred_element_type=F32,
        )[:1] * rescale

    ib_out[...] = pick(bsend[3, :, pl.ds(0, HALF)], x_hi * PAD + dp * 10)[:, :10]
    ob_out[...] = pick(bsend[3, :, pl.ds(HALF, D)], dp * 40)[:, :40]
    finish(0, skip5, gs_out)
    finish(2, inner5, gi_out)
    finish(1, outer5, go_out)
    for c in sent:
        c.wait_send()
    out0.wait()
    out1.wait()


N_SENDS = 136


def write_out(*refs):
    ins, outs, (big, grads, b10, b40, sem_in, sem_out) = refs[:6], refs[6:12], refs[12:]
    hops = [
        (ins[0].at[part(i, 80), :], big.at[part(i, 80), :], outs[0].at[part(i, 80), :])
        for i in range(4)
    ]
    hops += [(ins[i], grads.at[i - 1], outs[i]) for i in (1, 2, 3)]
    hops += [(ins[4], b10, outs[4]), (ins[5], b40, outs[5])]
    copies = []
    for i, (src, mid, dst) in enumerate(hops):
        c = pltpu.make_async_copy(src, mid, sem_in.at[i])
        c.start()
        copies.append((c, pltpu.make_async_copy(mid, dst, sem_out.at[i])))
    for a, b in copies:
        a.wait()
        b.start()
    for _, b in copies:
        b.wait()


def on_device(series, wi, ib, wo, ws, ob, targets, levels, counts):
    hbm = pl.BlockSpec(memory_space=pl.ANY)
    vmem = pl.BlockSpec(memory_space=pltpu.VMEM)
    smem = pl.BlockSpec(memory_space=pltpu.SMEM)
    grad = jax.ShapeDtypeStruct((C3, D), F32)
    shapes = (
        jax.ShapeDtypeStruct((SHARD, 2 * CHIP), F32), grad, grad, grad,
        jax.ShapeDtypeStruct((1, 10), F32), jax.ShapeDtypeStruct((1, 40), F32),
    )
    results = pl.pallas_call(
        kernel,
        out_shape=shapes,
        in_specs=[hbm] * 4 + [vmem] * 2 + [hbm] + [smem] * 2,
        out_specs=(hbm,) + (vmem,) * 5,
        scratch_shapes=[
            pltpu.VMEM((CHIP, D), BF16),
            pltpu.VMEM((HALF, D), BF16),
            pltpu.VMEM((HALF, D), BF16),
            pltpu.VMEM((HALF, D), BF16),
            pltpu.VMEM((1, HALF), F32),
            pltpu.VMEM((CORE, 128), F32),
            pltpu.VMEM((HALF, D), BF16),
            pltpu.VMEM((3, OWN, HALF), BF16),
            pltpu.VMEM((2, HALF, HALF), BF16),
            pltpu.VMEM((HALF, HALF), BF16),
            pltpu.VMEM((CHIP, HALF), BF16),
            pltpu.VMEM((CHIP, HALF), BF16),
            pltpu.VMEM((CHIP, HALF), F32),
            pltpu.VMEM((3, OWN, CHIP), BF16),
            pltpu.VMEM((2, CHIP, HALF), BF16),
            pltpu.VMEM((CHIP, D), BF16),
            pltpu.VMEM((CORE, D), F32),
            pltpu.VMEM((1, D), F32),
            pltpu.VMEM((5, CORE, 256), F32),
            pltpu.VMEM((5, CORE, 256), F32),
            pltpu.VMEM((CORE, D), F32),
            pltpu.VMEM((3, OWN, D), F32),
            pltpu.VMEM((3, OWN, D), BF16),
            pltpu.VMEM((3, 2, C1, LANES), BF16),
            pltpu.VMEM((3, 2, C1, LANES), BF16),
            pltpu.VMEM((3, 2, C1, LANES), BF16),
            pltpu.VMEM((3, 2, C1, LANES), BF16),
            pltpu.VMEM((3, C1, D), F32),
            pltpu.VMEM((3, 4, C2, D), BF16),
            pltpu.VMEM((3, 2, C2, LANES), BF16),
            pltpu.VMEM((3, 2, C2, LANES), BF16),
            pltpu.VMEM((3, 2, C2, LANES), BF16),
            pltpu.VMEM((3, 2, C2, LANES), BF16),
            pltpu.VMEM((3, C2, D), F32),
            pltpu.VMEM((3, 4, C3, D), F32),
            pltpu.VMEM((3, 4, C3, D), BF16),
            pltpu.VMEM((3, 3, C3, D), BF16),
            pltpu.VMEM((4, 1, HALF + D), F32),
            pltpu.VMEM((3, 3, 1, HALF + D), F32),
            pltpu.VMEM((HALF, CHIP), F32),
            pltpu.VMEM((SHARD, CHIP), BF16),
            pltpu.VMEM((SHARD, CHIP), BF16),
            pltpu.VMEM((SHARD, CHIP), BF16),
            pltpu.VMEM((SHARD, CHIP), F32),
            pltpu.SemaphoreType.DMA((8,)),
            pltpu.SemaphoreType.DMA((N_SENDS,)),
            pltpu.SemaphoreType.DMA((N_SENDS,)),
        ],
        compiler_params=pltpu.CompilerParams(
            collective_id=0, has_side_effects=True, vmem_limit_bytes=60 * 1024 * 1024
        ),
    )(series, wi, wo, ws, ib, ob, targets, levels, counts)
    input_grad, inner, outer, skip, inbias, outbias = pl.pallas_call(
        write_out,
        out_shape=shapes,
        in_specs=[hbm] * 6,
        out_specs=(hbm,) * 6,
        scratch_shapes=[
            pltpu.VMEM((SHARD, 2 * CHIP), F32),
            pltpu.VMEM((3, C3, D), F32),
            pltpu.VMEM((1, 10), F32),
            pltpu.VMEM((1, 40), F32),
            pltpu.SemaphoreType.DMA((9,)),
            pltpu.SemaphoreType.DMA((9,)),
        ],
    )(*results)
    return input_grad.T, inner, outer, skip, inbias.reshape(10), outbias.reshape(40)


def solution(mesh):
    return jax.shard_map(
        on_device,
        mesh=mesh,
        in_specs=(
            P("dp", None), P("mp", None), P("mp"), P("mp", None), P("mp", None), P(None),
            P("dp", None), P(None), P("dp"),
        ),
        out_specs=(
            P("dp", "mp"), P(("mp", "dp"), None), P(("mp", "dp"), None), P(("mp", "dp"), None),
            P(("mp", "dp")), P("dp"),
        ),
        check_vma=False,
    )
```

```python
import jax
import jax.numpy as jnp
from jax import lax
from jax.experimental import pallas as pl
from jax.experimental.pallas import tpu as pltpu
from jax.sharding import PartitionSpec as P

MESH = pl.DeviceIdType.MESH
F32 = jnp.float32
BF16 = jnp.bfloat16
LEVELS = 9
PATCHES = 16
QUANTILES = 10
HUBER_WIDTH = 0.5

D = 1280
SHARD = 320
PAD = 384
HALF = 2 * PAD
CHIP = 512
CORE = 256
OWN = 640
C1, C2, C3 = 160, 40, 10
LANES = 640

NN = (((1,), (0,)), ((), ()))
NT = (((1,), (1,)), ((), ()))
TT = (((0,), (1,)), ((), ()))


def mm(a, b, dims=NN):
    return lax.dot_general(a, b, dims, preferred_element_type=F32)


def rem(a, n):
    return lax.rem(a, jnp.int32(n))


def div(a, n):
    return lax.div(a, jnp.int32(n))


def part(index, size):
    return pl.ds(pl.multiple_of(index * size, size), size)


GROUPS = (("yxz", 0, 256), ("zyx", 512, 256), ("xzy", 1024, 128))


def split(n, size):
    q = (
        (n >= size).astype(jnp.int32)
        + (n >= 2 * size).astype(jnp.int32)
        + (n >= 3 * size).astype(jnp.int32)
    )
    return q, n - q * size


def natural(n, order):
    d1, n = split(n, C1)
    d2, n = split(n, C2)
    d3, r = split(n, C3)
    at = dict(zip(order, (d1, d2, d3)))
    x_hi = (at["x"] >= 2).astype(jnp.int32)
    x_lo = at["x"] - 2 * x_hi
    return x_hi * PAD + (at["z"] * 8 + x_lo * 4 + at["y"]) * 10 + r


def kernel(
    series_hbm, wi_hbm, wo_hbm, ws_hbm, ib_ref, ob_ref, targets_hbm, levels_ref, counts_ref,
    in_out, gi_out, go_out, gs_out, ib_out, ob_out,
    S, Wi, Wo, Ws, IB, T, sel, perm, sH, H, DV, LT, HG, OG,
    spread, tau, p_send, p_recv, p_own, G, ST, RA, RD, RSUM, T2,
    acc1, ST2, RA2, RD2, RSUM2, T3, acc2, F3, ST3, R3,
    bsend, brecv, igp, igp_recv, igf, ig_send, ig_mid, ig_recv,
    lsem, ssem, rsem,
):
    dp = lax.axis_index("dp")
    mp = lax.axis_index("mp")
    core = rem(mp, 2)
    x_hi = div(mp, 2)
    z = div(dp, 8)
    x_lo = rem(div(dp, 4), 2)
    y = rem(dp, 4)
    x = x_hi * 2 + x_lo
    other_hi = 1 - x_hi

    def device(x, y, z, core):
        return {"dp": z * 8 + rem(x, 2) * 4 + y, "mp": div(x, 2) * 2 + core}

    pos = {"x": x, "y": y, "z": z}

    def along(axis, k):
        at = dict(pos)
        at[axis] = rem(at[axis] + k, 4)
        return device(at["x"], at["y"], at["z"], core)

    partner = device(x, y, z, 1 - core)
    cross = device(3 - x, y, z, core)
    beside = device(x + 1 - 2 * x_lo, y, z, core)

    loads = []

    def load(src, dst):
        c = pltpu.make_async_copy(src, dst, lsem.at[len(loads)])
        c.start()
        loads.append(c)
        return c

    own_rows = pl.ds(pl.multiple_of(x_hi * PAD, 128), SHARD)
    l_i = load(wi_hbm, Wi.at[own_rows, :])
    l_s = load(ws_hbm, Ws.at[own_rows, :])
    l_o = load(wo_hbm, Wo.at[own_rows, :])
    l_series = load(series_hbm.at[part(x_hi, CHIP), :], S)
    l_t = load(targets_hbm.at[part(x_hi * 2 + core, CORE), :], T)

    IB[:, part(x_hi, PAD)] = jnp.concatenate(
        [ib_ref[...].reshape(1, SHARD), jnp.zeros((1, PAD - SHARD), F32)], axis=1
    )
    barrier = pltpu.get_barrier_semaphore()
    peers = [partner] + [along(a, k) for a in "xyz" for k in (1, 2, 3)]
    for peer in peers:
        pl.semaphore_signal(barrier, inc=1, device_id=peer, device_id_type=MESH)
    pl.semaphore_wait(barrier, len(peers))

    sent = []

    def send(src, dst, to):
        i = len(sent)
        c = pltpu.make_async_remote_copy(
            src_ref=src, dst_ref=dst, send_sem=ssem.at[i], recv_sem=rsem.at[i],
            device_id=to, device_id_type=MESH,
        )
        c.start()
        sent.append(c)
        return c

    weights = (Wi, Ws, Wo)
    axis_of = (y, z)

    def quarter(w, hi, color, q, start, size):
        return weights[w].at[
            pl.ds(pl.multiple_of(hi * PAD + q * 80, 16), 80),
            pl.ds(pl.multiple_of(color * LANES + start, 128), size),
        ]

    def on_color(color, a, b):
        return jnp.where(color == 0, a, b)

    first, second = x_lo, 1 - x_lo

    def ring(color):
        up = {k: on_color(color, along("y", 1)[k], along("z", 1)[k]) for k in ("dp", "mp")}
        down = {k: on_color(color, along("y", 3)[k], along("z", 3)[k]) for k in ("dp", "mp")}
        return on_color(color, y, z), up, down

    items = [
        (w, start, size, cut)
        for w in range(3)
        for start, size, cut in ((0, 384, 256 - 128 * (w % 2)), (384, 256, 128))
    ]
    crossed, beside_of, own_of, relayed = [], {}, {}, {}
    for i, (w, start, size, _) in enumerate(items):
        if i % 2 == 0:
            (l_i, l_s, l_o)[w].wait()
        piece = quarter(w, x_hi, second, on_color(second, y, z), start, size)
        crossed.append(send(piece, piece, cross))
        if w == 2:
            piece = quarter(w, x_hi, first, on_color(first, y, z), start, size)
            beside_of[i] = send(piece, piece, cross)
        if i == 1:
            own_bias = IB.at[:, part(x_hi, PAD)]
            b_crossed = send(own_bias, own_bias, cross)

    for W in weights:
        for j in range(2):
            W[pl.ds(j * PAD + SHARD, PAD - SHARD), :] = jnp.zeros((PAD - SHARD, D), BF16)

    def one_hot_sel(k):
        def body(i, _):
            h = lax.broadcasted_iota(jnp.int32, (128, D), 0) + i * 128
            col = lax.broadcasted_iota(jnp.int32, (128, D), 1)
            hi = (h >= PAD).astype(jnp.int32)
            j = h - hi * PAD
            want = hi * 640 + k * SHARD + j
            sel[part(i, 128), :] = jnp.where((col == want) & (j < SHARD), 1.0, 0.0).astype(BF16)
            return 0

        lax.fori_loop(0, HALF // 128, body, 0)

    def forward_first(i):
        w, start, size, _ = items[i]
        q, up, down = ring(first)
        crossed[i].wait_recv()
        piece = quarter(w, other_hi, first, q, start, size)
        if w < 2:
            beside_of[i] = send(piece, piece, beside)
        own_of[i, 0] = send(piece, piece, up), send(piece, piece, down)

    def forward_second(i):
        w, start, size, _ = items[i]
        q, up, down = ring(second)
        beside_of[i].wait_recv()
        piece = quarter(w, other_hi, second, q, start, size)
        own_of[i, 1] = send(piece, piece, up), send(piece, piece, down)

    def relay(i, turn):
        w, start, size, cut = items[i]
        color = (first, second)[turn]
        q, up, down = ring(color)
        from_below, from_above = own_of[i, turn]
        from_below.wait_recv()
        a = quarter(w, other_hi, color, rem(q + 3, 4), start, cut)
        s1 = send(a, a, up)
        from_above.wait_recv()
        b = quarter(w, other_hi, color, rem(q + 1, 4), start + cut, size - cut)
        relayed[i, turn] = s1, send(b, b, down)

    def arrived(i):
        for turn in range(2):
            for c in relayed[i, turn]:
                c.wait_recv()

    def sel_body(i, _):
        sH[:, part(i, 256)] = mm(S[...], sel[part(i, 256), :], NT).astype(BF16)
        return 0

    def make_perm(k):
        def body(i, _):
            n = lax.broadcasted_iota(jnp.int32, (128, 128), 0) + i * 128
            want = natural(n, GROUPS[k][0])
            lane = lax.broadcasted_iota(jnp.int32, (128, 128), 1)
            for t in range(HALF // 128):
                perm[k, part(i, 128), pl.ds(t * 128, 128)] = jnp.where(
                    lane + t * 128 == want, 1.0, 0.0
                ).astype(BF16)
            return 0

        lax.fori_loop(0, OWN // 128, body, 0)

    def transposed(k, g, src):
        def body(i, _):
            LT[k, g, :, part(i, 256)] = mm(perm[g], src[part(i, 256), :], NT).astype(BF16)
            return 0

        lax.fori_loop(0, CHIP // 256, body, 0, unroll=True)

    def spread_body(i, _):
        cols = part(i, 256)
        col = lax.broadcasted_iota(jnp.int32, (128, 256), 1) + i * 256
        row = lax.broadcasted_iota(jnp.int32, (128, 256), 0)
        off = col - row * QUANTILES
        spreader = jnp.where((off >= 0) & (off < QUANTILES), 1.0, 0.0).astype(F32)
        spread[:, cols] = (
            lax.dot_general(
                T[...], spreader, NN, precision=lax.Precision.HIGHEST, preferred_element_type=F32
            )
            - p_own[:1, cols]
        )
        rows = jnp.zeros((128, 256), F32)
        for c in range(QUANTILES):
            level = jnp.full((128, 256), levels_ref[c], jnp.int32).astype(F32) + 1.0
            rows = rows + jnp.where(off == c, level / (LEVELS + 1), 0.0)
        tau[:, cols] = jnp.sum(rows, axis=0, keepdims=True)
        return 0

    def hidden_body(i, _):
        cols = part(i, 256)
        pre = mm(S[...], Wi[cols, :], NT) + IB[:, cols]
        sig = jax.nn.sigmoid(pre)
        H[:, cols] = (pre * sig).astype(BF16)
        DV[:, cols] = sig * (1.0 + pre * (1.0 - sig))
        return 0

    one_hot_sel(core)
    l_series.wait()
    p_own[:1, :] = ob_ref[...].reshape(1, D)
    lax.fori_loop(0, 3, sel_body, 0)
    forward_first(0)
    make_perm(0)
    forward_first(1)
    make_perm(1)
    forward_first(2)
    make_perm(2)
    forward_first(3)
    forward_second(0)
    relay(0, 0)
    transposed(0, 0, sH)
    forward_first(4)
    forward_second(1)
    relay(1, 0)
    l_t.wait()
    lax.fori_loop(0, 2, spread_body, 0)
    forward_first(5)
    forward_second(2)
    relay(2, 0)
    lax.fori_loop(2, 5, spread_body, 0)
    forward_second(3)
    relay(3, 0)
    relay(0, 1)
    transposed(0, 1, sH)
    forward_second(4)
    relay(4, 0)
    relay(1, 1)
    forward_second(5)
    relay(5, 0)
    relay(2, 1)
    transposed(0, 2, sH)
    arrived(0)
    arrived(1)
    b_crossed.wait_recv()
    relay(3, 1)
    lax.fori_loop(0, 2, hidden_body, 0, unroll=True)
    relay(4, 1)
    lax.fori_loop(2, 3, hidden_body, 0)
    relay(5, 1)
    transposed(1, 0, H)
    for i in range(2, 6):
        arrived(i)

    mine, theirs = part(core, CORE), part(1 - core, CORE)

    def predict(rows, cols):
        return mm(H[rows, :], Wo[:, cols]) + mm(sH[rows, :], Ws[:, cols])

    p_copies = []
    for i in range(D // 256):
        cols = pl.ds(i * 256, 256)
        p_send[i] = predict(theirs, cols)
        p_copies.append(send(p_send.at[i], p_recv.at[i], partner))

    def predict_body(i, _):
        cols = part(i, 256)
        p_own[:, cols] = predict(mine, cols)
        return 0

    lax.fori_loop(0, D // 256, predict_body, 0, unroll=True)
    transposed(1, 1, H)
    transposed(1, 2, H)
    for c in p_copies:
        c.wait_recv()

    def slope_body(w, _):
        rows = part(w, PATCHES)
        count = counts_ref[(x_hi * 2 + core) * (CORE // PATCHES) + w]
        counted = jnp.full((PATCHES, 128), count, jnp.int32)
        valid = lax.broadcasted_iota(jnp.int32, (PATCHES, 128), 0) < counted
        weight = (jnp.where(valid, 1.0, 0.0) / counted.astype(F32))[:, :1]
        for i in range(D // 256):
            cols = pl.ds(i * 256, 256)
            residue = spread[rows, cols] - (p_own[rows, cols] + p_recv[i, rows, :])
            t = tau[:, cols]
            slopes = jnp.where(residue >= 0, t, 1.0 - t) * jnp.clip(
                residue / HUBER_WIDTH, -1.0, 1.0
            )
            OG[pl.ds(pl.multiple_of(core * CORE + w * PATCHES, PATCHES), PATCHES), cols] = (
                -slopes * weight
            ).astype(BF16)
        return 0

    og_copies = []
    for i in range(2):
        lax.fori_loop(8 * i, 8 * i + 8, slope_body, 0)
        rows = OG.at[part(core * 2 + i, 128), :]
        og_copies.append(send(rows, rows, partner))

    def backflow(rows):
        def body(i, _):
            cols = part(i, 256)
            back = mm(OG[rows, :], Wo[cols, :], NT)
            HG[rows, cols] = (back * DV[rows, cols]).astype(BF16)
            return 0

        lax.fori_loop(0, HALF // 256, body, 0, unroll=True)

    backflow(mine)
    for c in og_copies:
        c.wait_recv()

    def lanes(g, h):
        return pl.ds(GROUPS[g][1] + h * GROUPS[g][2], GROUPS[g][2])

    def half_lanes(g):
        return pl.ds(GROUPS[g][1] // 2, GROUPS[g][2])

    def ring_start(axis, g, view, ra, rd):
        p = pos[axis]
        up, down = along(axis, 1), along(axis, 3)
        to = half_lanes(g)
        return (
            send(view(rem(p + 2, 4), lanes(g, 0)), ra.at[0, :, to], up),
            send(view(rem(p + 2, 4), lanes(g, 1)), ra.at[1, :, to], down),
            send(view(rem(p + 1, 4), lanes(g, 1)), rd.at[0, :, to], up),
            send(view(rem(p + 3, 4), lanes(g, 0)), rd.at[1, :, to], down),
        )

    def ring_pass(axis, g, size, rows, base, ra, out, rsum, own, step):
        p = pos[axis]
        to = half_lanes(g)
        passed = []
        for h, hop in ((0, 1), (1, 3)):
            step[h].wait_recv()

            def body(i, _, h=h, hop=hop):
                there = pl.ds(
                    pl.multiple_of(base + rem(p + hop, 4) * size + i * rows, 8), rows
                )
                here = part(i, rows)
                out[h, here, to] = (
                    own[there, lanes(g, h)] + ra[h, here, to].astype(F32)
                ).astype(BF16)
                return 0

            lax.fori_loop(0, size // rows, body, 0)
            passed.append(send(out.at[h, :, to], rsum.at[h, :, to], along(axis, hop)))
        return passed

    def ring_end(axis, g, size, rows, base, rsum, rd, own, dst, step, passed):
        p = pos[axis]
        to = half_lanes(g)
        for c in (step[2], step[3], passed[0], passed[1]):
            c.wait_recv()

        def body(i, _):
            there = pl.ds(pl.multiple_of(base + p * size + i * rows, 8), rows)
            here = part(i, rows)
            for h in range(2):
                dst[here, lanes(g, h)] = (
                    own[there, lanes(g, h)]
                    + rsum[h, here, to].astype(F32)
                    + rd[1 - h, here, to].astype(F32)
                )
            return 0

        lax.fori_loop(0, size // rows, body, 0)

    steps = {}

    def gradient(k, right):
        for g, (order, start, width) in enumerate(GROUPS):
            def body(i, _, g=g):
                cols = part(i, 256)
                value = mm(LT[k, g], right[:, cols])
                G[k, :, cols] = value
                ST[k, :, cols] = value.astype(BF16)
                return 0

            lax.fori_loop(start // 256, (start + 2 * width) // 256, body, 0, unroll=True)
            steps[k, g, 0] = ring_start(
                order[0], g, lambda q, cols: ST.at[k, part(q, C1), cols], RA.at[k], RD.at[k]
            )

    def pass_on(k):
        for g, (order, _, _) in enumerate(GROUPS):
            steps[k, g, 1] = ring_pass(
                order[0], g, C1, 32, 0, RA.at[k], T2.at[k], RSUM.at[k], G.at[k], steps[k, g, 0]
            )

    def second_phase(k):
        for g, (order, start, width) in enumerate(GROUPS):
            ring_end(
                order[0], g, C1, 32, 0, RSUM.at[k], RD.at[k], G.at[k], acc1.at[k],
                steps[k, g, 0], steps[k, g, 1],
            )
            cols = pl.ds(start, 2 * width)
            for q in range(4):
                ST2[k, q, :, cols] = acc1[k, pl.ds(q * C2, C2), cols].astype(BF16)
            steps[k, g, 2] = ring_start(
                order[1], g, lambda q, cols: ST2.at[k, q, :, cols], RA2.at[k], RD2.at[k]
            )

    def pass_on_second(k):
        for g, (order, _, _) in enumerate(GROUPS):
            steps[k, g, 3] = ring_pass(
                order[1], g, C2, C2, 0, RA2.at[k], T3.at[k], RSUM2.at[k], acc1.at[k],
                steps[k, g, 2],
            )

    def third_phase(k):
        for g, (order, start, width) in enumerate(GROUPS):
            ring_end(
                order[1], g, C2, C2, 0, RSUM2.at[k], RD2.at[k], acc1.at[k], acc2.at[k],
                steps[k, g, 2], steps[k, g, 3],
            )
            cols = pl.ds(start, 2 * width)
            for q in range(4):
                piece = acc2[k, pl.ds(q * C3, C3), cols]
                F3[k, q, :, cols] = piece
                ST3[k, q, :, cols] = piece.astype(BF16)
            p3 = pos[order[2]]
            steps[k, g, 4] = [
                send(
                    ST3.at[k, rem(p3 + o, 4), :, cols], R3.at[k, o - 1, :, cols],
                    along(order[2], o),
                )
                for o in (1, 3, 2)
            ]

    rescale = 1.0 / 2048

    def finish(k, out):
        for g, (order, start, width) in enumerate(GROUPS):
            for c in steps[k, g, 4]:
                c.wait_recv()
            cols = pl.ds(start, 2 * width)
            total = F3[k, pos[order[2]], :, cols]
            for o in range(3):
                total = total + R3[k, o, :, cols].astype(F32)
            out[:, cols] = total * rescale

    gradient(0, OG)
    gradient(1, OG)
    backflow(theirs)
    for g in range(3):
        transposed(2, g, HG)
    pass_on(0)
    gradient(2, S)
    pass_on(1)

    bsend[0, :, pl.ds(0, HALF)] = jnp.sum(HG[...].astype(F32), axis=0, keepdims=True)
    bsend[0, :, pl.ds(HALF, D)] = jnp.sum(OG[...].astype(F32), axis=0, keepdims=True)

    def bias_send(i):
        axis = "xyz"[i]
        return [send(bsend.at[i], brecv.at[i, o - 1], along(axis, o)) for o in (1, 2, 3)]

    def bias_add(i, copies):
        for c in copies:
            c.wait_recv()
        bsend[i + 1] = bsend[i] + brecv[i, 0] + brecv[i, 1] + brecv[i, 2]

    bias1 = bias_send(0)
    for i in range(CHIP // 256):
        rows = pl.ds(i * 256, 256)
        igp[:, rows] = mm(Wi[...], HG[rows, :], TT)
    igp_copies = []
    for j in range(2):
        rows = pl.ds(pl.multiple_of(j * 640 + (1 - core) * SHARD, 64), SHARD)
        igp_copies.append(send(igp.at[rows, :], igp_recv.at[j], partner))
    second_phase(0)
    pass_on(2)
    for i in range(CHIP // 256):
        rows = pl.ds(i * 256, 256)
        igf[:, rows] = mm(Ws[...], OG[rows, :], NT)
    for c in igp_copies:
        c.wait_recv()

    def columns(hi):
        here = pl.ds(pl.multiple_of(hi * PAD, 128), SHARD)
        there = pl.ds(pl.multiple_of(hi * 640 + core * SHARD, 64), SHARD)
        return igf[here, :] + igp[there, :] + igp_recv[hi]

    ig_send[...] = columns(other_hi).astype(BF16)
    igf[own_rows, :] = columns(x_hi)
    lower, upper = pl.ds(0, SHARD // 2), pl.ds(SHARD // 2, SHARD // 2)
    ig1 = (
        send(ig_send.at[lower, :], ig_mid.at[lower, :], along("x", 1)),
        send(ig_send.at[upper, :], ig_mid.at[upper, :], along("x", 3)),
    )
    out0 = pltpu.make_async_copy(
        igf.at[own_rows, :], in_out.at[:, part(x_hi, CHIP)], lsem.at[len(loads)]
    )
    out0.start()
    second_phase(1)
    bias_add(0, bias1)
    bias2 = bias_send(1)
    pass_on_second(0)
    second_phase(2)
    pass_on_second(1)
    third_phase(0)
    for c in ig1:
        c.wait_recv()
    ig2 = (
        send(ig_mid.at[lower, :], ig_recv.at[lower, :], along("x", 1)),
        send(ig_mid.at[upper, :], ig_recv.at[upper, :], along("x", 3)),
    )
    pass_on_second(2)
    bias_add(1, bias2)
    bias3 = bias_send(2)
    third_phase(1)
    third_phase(2)
    for c in ig2:
        c.wait_recv()
    others = pl.ds(pl.multiple_of(other_hi * PAD, 128), SHARD)
    igf[others, :] = ig_recv[...].astype(F32)
    out1 = pltpu.make_async_copy(
        igf.at[others, :], in_out.at[:, part(other_hi, CHIP)], lsem.at[len(loads) + 1]
    )
    out1.start()
    bias_add(2, bias3)

    def pick(v, start):
        n = v.shape[1]
        i = lax.broadcasted_iota(jnp.int32, (n, 128), 0)
        j = lax.broadcasted_iota(jnp.int32, (n, 128), 1)
        hot = jnp.where(i == j + start, 1.0, 0.0).astype(F32)
        return lax.dot_general(
            jnp.broadcast_to(v, (8, n)), hot, NN,
            precision=lax.Precision.HIGHEST, preferred_element_type=F32,
        )[:1] * rescale

    ib_out[...] = pick(bsend[3, :, pl.ds(0, HALF)], x_hi * PAD + dp * 10)[:, :10]
    ob_out[...] = pick(bsend[3, :, pl.ds(HALF, D)], dp * 40)[:, :40]
    finish(0, gs_out)
    finish(1, go_out)
    finish(2, gi_out)
    assert len(sent) == N_SENDS
    for c in sent:
        c.wait_send()
    out0.wait()
    out1.wait()


N_SENDS = 218


def write_out(*refs):
    ins, outs, (big, grads, b10, b40, sem_in, sem_out) = refs[:6], refs[6:12], refs[12:]
    hops = [
        (ins[0].at[part(i, 80), :], big.at[part(i, 80), :], outs[0].at[part(i, 80), :])
        for i in range(4)
    ]
    hops += [(ins[i], grads.at[i - 1], outs[i]) for i in (1, 2, 3)]
    hops += [(ins[4], b10, outs[4]), (ins[5], b40, outs[5])]
    copies = []
    for i, (src, mid, dst) in enumerate(hops):
        c = pltpu.make_async_copy(src, mid, sem_in.at[i])
        c.start()
        copies.append((c, pltpu.make_async_copy(mid, dst, sem_out.at[i])))
    for a, b in copies:
        a.wait()
        b.start()
    for _, b in copies:
        b.wait()


def on_device(series, wi, ib, wo, ws, ob, targets, levels, counts):
    hbm = pl.BlockSpec(memory_space=pl.ANY)
    vmem = pl.BlockSpec(memory_space=pltpu.VMEM)
    smem = pl.BlockSpec(memory_space=pltpu.SMEM)
    grad = jax.ShapeDtypeStruct((C3, D), F32)
    shapes = (
        jax.ShapeDtypeStruct((SHARD, 2 * CHIP), F32), grad, grad, grad,
        jax.ShapeDtypeStruct((1, 10), F32), jax.ShapeDtypeStruct((1, 40), F32),
    )
    results = pl.pallas_call(
        kernel,
        out_shape=shapes,
        in_specs=[hbm] * 4 + [vmem] * 2 + [hbm] + [smem] * 2,
        out_specs=(hbm,) + (vmem,) * 5,
        scratch_shapes=[
            pltpu.VMEM((CHIP, D), BF16),
            pltpu.VMEM((HALF, D), BF16),
            pltpu.VMEM((HALF, D), BF16),
            pltpu.VMEM((HALF, D), BF16),
            pltpu.VMEM((1, HALF), F32),
            pltpu.VMEM((CORE, 128), F32),
            pltpu.VMEM((HALF, D), BF16),
            pltpu.VMEM((3, OWN, HALF), BF16),
            pltpu.VMEM((CHIP, HALF), BF16),
            pltpu.VMEM((CHIP, HALF), BF16),
            pltpu.VMEM((CHIP, HALF), F32),
            pltpu.VMEM((3, 3, OWN, CHIP), BF16),
            pltpu.VMEM((CHIP, HALF), BF16),
            pltpu.VMEM((CHIP, D), BF16),
            pltpu.VMEM((CORE, D), F32),
            pltpu.VMEM((1, D), F32),
            pltpu.VMEM((5, CORE, 256), F32),
            pltpu.VMEM((5, CORE, 256), F32),
            pltpu.VMEM((CORE, D), F32),
            pltpu.VMEM((3, OWN, D), F32),
            pltpu.VMEM((3, OWN, D), BF16),
            pltpu.VMEM((3, 2, C1, LANES), BF16),
            pltpu.VMEM((3, 2, C1, LANES), BF16),
            pltpu.VMEM((3, 2, C1, LANES), BF16),
            pltpu.VMEM((3, 2, C1, LANES), BF16),
            pltpu.VMEM((3, C1, D), F32),
            pltpu.VMEM((3, 4, C2, D), BF16),
            pltpu.VMEM((3, 2, C2, LANES), BF16),
            pltpu.VMEM((3, 2, C2, LANES), BF16),
            pltpu.VMEM((3, 2, C2, LANES), BF16),
            pltpu.VMEM((3, 2, C2, LANES), BF16),
            pltpu.VMEM((3, C2, D), F32),
            pltpu.VMEM((3, 4, C3, D), F32),
            pltpu.VMEM((3, 4, C3, D), BF16),
            pltpu.VMEM((3, 3, C3, D), BF16),
            pltpu.VMEM((4, 1, HALF + D), F32),
            pltpu.VMEM((3, 3, 1, HALF + D), F32),
            pltpu.VMEM((D, CHIP), F32),
            pltpu.VMEM((2, SHARD, CHIP), F32),
            pltpu.VMEM((HALF, CHIP), F32),
            pltpu.VMEM((SHARD, CHIP), BF16),
            pltpu.VMEM((SHARD, CHIP), BF16),
            pltpu.VMEM((SHARD, CHIP), BF16),
            pltpu.SemaphoreType.DMA((8,)),
            pltpu.SemaphoreType.DMA((N_SENDS,)),
            pltpu.SemaphoreType.DMA((N_SENDS,)),
        ],
        compiler_params=pltpu.CompilerParams(
            collective_id=0, has_side_effects=True, vmem_limit_bytes=63 * 1024 * 1024
        ),
    )(series, wi, wo, ws, ib, ob, targets, levels, counts)
    input_grad, inner, outer, skip, inbias, outbias = pl.pallas_call(
        write_out,
        out_shape=shapes,
        in_specs=[hbm] * 6,
        out_specs=(hbm,) * 6,
        scratch_shapes=[
            pltpu.VMEM((SHARD, 2 * CHIP), F32),
            pltpu.VMEM((3, C3, D), F32),
            pltpu.VMEM((1, 10), F32),
            pltpu.VMEM((1, 40), F32),
            pltpu.SemaphoreType.DMA((9,)),
            pltpu.SemaphoreType.DMA((9,)),
        ],
    )(*results)
    return input_grad.T, inner, outer, skip, inbias.reshape(10), outbias.reshape(40)


def solution(mesh):
    return jax.shard_map(
        on_device,
        mesh=mesh,
        in_specs=(
            P("dp", None), P("mp", None), P("mp"), P("mp", None), P("mp", None), P(None),
            P("dp", None), P(None), P("dp"),
        ),
        out_specs=(
            P("dp", "mp"), P(("mp", "dp"), None), P(("mp", "dp"), None), P(("mp", "dp"), None),
            P(("mp", "dp")), P("dp"),
        ),
        check_vma=False,
    )
```

```python
import jax
import jax.numpy as jnp
from jax import lax
from jax.experimental import pallas as pl
from jax.experimental.pallas import tpu as pltpu
from jax.sharding import PartitionSpec as P

MESH = pl.DeviceIdType.MESH
F32 = jnp.float32
BF16 = jnp.bfloat16
LEVELS = 9
PATCHES = 16
QUANTILES = 10
HUBER_WIDTH = 0.5

D = 1280
SHARD = 320
PAD = 384
HALF = 2 * PAD
CHIP = 512
CORE = 256
OWN = 640
C1, C2, C3 = 160, 40, 10
LANES = 640

NN = (((1,), (0,)), ((), ()))
NT = (((1,), (1,)), ((), ()))
TT = (((0,), (1,)), ((), ()))


def mm(a, b, dims=NN):
    return lax.dot_general(a, b, dims, preferred_element_type=F32)


def rem(a, n):
    return lax.rem(a, jnp.int32(n))


def div(a, n):
    return lax.div(a, jnp.int32(n))


def part(index, size):
    return pl.ds(pl.multiple_of(index * size, size), size)


GROUPS = (("yxz", 0, 256), ("zyx", 512, 256), ("xzy", 1024, 128))


def split(n, size):
    q = (
        (n >= size).astype(jnp.int32)
        + (n >= 2 * size).astype(jnp.int32)
        + (n >= 3 * size).astype(jnp.int32)
    )
    return q, n - q * size


def natural(n, order):
    d1, n = split(n, C1)
    d2, n = split(n, C2)
    d3, r = split(n, C3)
    at = dict(zip(order, (d1, d2, d3)))
    x_hi = (at["x"] >= 2).astype(jnp.int32)
    x_lo = at["x"] - 2 * x_hi
    return x_hi * PAD + (at["z"] * 8 + x_lo * 4 + at["y"]) * 10 + r


def kernel(
    series_hbm, wi_hbm, wo_hbm, ws_hbm, ib_ref, ob_ref, targets_hbm, levels_ref, counts_ref,
    in_out, gi_out, go_out, gs_out, ib_out, ob_out,
    S, Wi, Wo, Ws, IB, T, sel, perm, sH, H, DV, LT, HG, OG,
    spread, tau, p_send, p_recv, p_own, G, ST, RA, RD, RSUM, T2,
    acc1, ST2, RA2, RD2, RSUM2, T3, acc2, F3, ST3, R3,
    bsend, brecv, igp, igp_recv, igf, ig_send, ig_mid, ig_recv,
    lsem, ssem, rsem,
):
    dp = lax.axis_index("dp")
    mp = lax.axis_index("mp")
    core = rem(mp, 2)
    x_hi = div(mp, 2)
    z = div(dp, 8)
    x_lo = rem(div(dp, 4), 2)
    y = rem(dp, 4)
    x = x_hi * 2 + x_lo
    other_hi = 1 - x_hi

    def device(x, y, z, core):
        return {"dp": z * 8 + rem(x, 2) * 4 + y, "mp": div(x, 2) * 2 + core}

    pos = {"x": x, "y": y, "z": z}

    def along(axis, k):
        at = dict(pos)
        at[axis] = rem(at[axis] + k, 4)
        return device(at["x"], at["y"], at["z"], core)

    partner = device(x, y, z, 1 - core)
    cross = device(3 - x, y, z, core)
    beside = device(x + 1 - 2 * x_lo, y, z, core)

    loads = []

    def load(src, dst):
        c = pltpu.make_async_copy(src, dst, lsem.at[len(loads)])
        c.start()
        loads.append(c)
        return c

    own_rows = pl.ds(pl.multiple_of(x_hi * PAD, 128), SHARD)
    l_i = load(wi_hbm, Wi.at[own_rows, :])
    l_s = load(ws_hbm, Ws.at[own_rows, :])
    l_o = load(wo_hbm, Wo.at[own_rows, :])
    l_series = load(series_hbm.at[part(x_hi, CHIP), :], S)
    l_t = load(targets_hbm.at[part(x_hi * 2 + core, CORE), :], T)

    IB[:, part(x_hi, PAD)] = jnp.concatenate(
        [ib_ref[...].reshape(1, SHARD), jnp.zeros((1, PAD - SHARD), F32)], axis=1
    )
    barrier = pltpu.get_barrier_semaphore()
    peers = [partner] + [along(a, k) for a in "xyz" for k in (1, 2, 3)]
    for peer in peers:
        pl.semaphore_signal(barrier, inc=1, device_id=peer, device_id_type=MESH)
    pl.semaphore_wait(barrier, len(peers))

    sent = []

    def send(src, dst, to):
        i = len(sent)
        c = pltpu.make_async_remote_copy(
            src_ref=src, dst_ref=dst, send_sem=ssem.at[i], recv_sem=rsem.at[i],
            device_id=to, device_id_type=MESH,
        )
        c.start()
        sent.append(c)
        return c

    weights = (Wi, Ws, Wo)
    axis_of = (y, z)

    def quarter(w, hi, color, q, start, size):
        return weights[w].at[
            pl.ds(pl.multiple_of(hi * PAD + q * 80, 16), 80),
            pl.ds(pl.multiple_of(color * LANES + start, 128), size),
        ]

    def on_color(color, a, b):
        return jnp.where(color == 0, a, b)

    first, second = x_lo, 1 - x_lo

    def ring(color):
        up = {k: on_color(color, along("y", 1)[k], along("z", 1)[k]) for k in ("dp", "mp")}
        down = {k: on_color(color, along("y", 3)[k], along("z", 3)[k]) for k in ("dp", "mp")}
        return on_color(color, y, z), up, down

    items = [
        (w, start, size, cut)
        for w in range(3)
        for start, size, cut in ((0, 384, 256 - 128 * (w % 2)), (384, 256, 128))
    ]
    crossed, beside_of, own_of, relayed = [], {}, {}, {}
    for i, (w, start, size, _) in enumerate(items):
        if i % 2 == 0:
            (l_i, l_s, l_o)[w].wait()
        piece = quarter(w, x_hi, second, on_color(second, y, z), start, size)
        crossed.append(send(piece, piece, cross))
        if w == 2:
            piece = quarter(w, x_hi, first, on_color(first, y, z), start, size)
            beside_of[i] = send(piece, piece, cross)
        if i == 1:
            own_bias = IB.at[:, part(x_hi, PAD)]
            b_crossed = send(own_bias, own_bias, cross)

    for W in weights:
        for j in range(2):
            W[pl.ds(j * PAD + SHARD, PAD - SHARD), :] = jnp.zeros((PAD - SHARD, D), BF16)

    def one_hot_sel(k):
        def body(i, _):
            h = lax.broadcasted_iota(jnp.int32, (128, D), 0) + i * 128
            col = lax.broadcasted_iota(jnp.int32, (128, D), 1)
            hi = (h >= PAD).astype(jnp.int32)
            j = h - hi * PAD
            want = hi * 640 + k * SHARD + j
            sel[part(i, 128), :] = jnp.where((col == want) & (j < SHARD), 1.0, 0.0).astype(BF16)
            return 0

        lax.fori_loop(0, HALF // 128, body, 0)

    def forward_first(i):
        w, start, size, _ = items[i]
        q, up, down = ring(first)
        crossed[i].wait_recv()
        piece = quarter(w, other_hi, first, q, start, size)
        if w < 2:
            beside_of[i] = send(piece, piece, beside)
        own_of[i, 0] = send(piece, piece, up), send(piece, piece, down)

    def forward_second(i):
        w, start, size, _ = items[i]
        q, up, down = ring(second)
        beside_of[i].wait_recv()
        piece = quarter(w, other_hi, second, q, start, size)
        own_of[i, 1] = send(piece, piece, up), send(piece, piece, down)

    def relay(i, turn):
        w, start, size, cut = items[i]
        color = (first, second)[turn]
        q, up, down = ring(color)
        from_below, from_above = own_of[i, turn]
        from_below.wait_recv()
        a = quarter(w, other_hi, color, rem(q + 3, 4), start, cut)
        s1 = send(a, a, up)
        from_above.wait_recv()
        b = quarter(w, other_hi, color, rem(q + 1, 4), start + cut, size - cut)
        relayed[i, turn] = s1, send(b, b, down)

    def arrived(i):
        for turn in range(2):
            for c in relayed[i, turn]:
                c.wait_recv()

    def sel_body(i, _):
        sH[:, part(i, 256)] = mm(S[...], sel[part(i, 256), :], NT).astype(BF16)
        return 0

    def make_perm(k):
        def body(i, _):
            n = lax.broadcasted_iota(jnp.int32, (128, 128), 0) + i * 128
            want = natural(n, GROUPS[k][0])
            lane = lax.broadcasted_iota(jnp.int32, (128, 128), 1)
            for t in range(HALF // 128):
                perm[k, part(i, 128), pl.ds(t * 128, 128)] = jnp.where(
                    lane + t * 128 == want, 1.0, 0.0
                ).astype(BF16)
            return 0

        lax.fori_loop(0, OWN // 128, body, 0)

    def transposed(k, g, src):
        def body(i, _):
            LT[k, g, :, part(i, 256)] = mm(perm[g], src[part(i, 256), :], NT).astype(BF16)
            return 0

        lax.fori_loop(0, CHIP // 256, body, 0, unroll=True)

    def spread_body(i, _):
        cols = part(i, 256)
        col = lax.broadcasted_iota(jnp.int32, (128, 256), 1) + i * 256
        row = lax.broadcasted_iota(jnp.int32, (128, 256), 0)
        off = col - row * QUANTILES
        spreader = jnp.where((off >= 0) & (off < QUANTILES), 1.0, 0.0).astype(F32)
        spread[:, cols] = (
            lax.dot_general(
                T[...], spreader, NN, precision=lax.Precision.HIGHEST, preferred_element_type=F32
            )
            - p_own[:1, cols]
        )
        rows = jnp.zeros((128, 256), F32)
        for c in range(QUANTILES):
            level = jnp.full((128, 256), levels_ref[c], jnp.int32).astype(F32) + 1.0
            rows = rows + jnp.where(off == c, level / (LEVELS + 1), 0.0)
        tau[:, cols] = jnp.sum(rows, axis=0, keepdims=True)
        return 0

    def hidden_body(i, _):
        cols = part(i, 256)
        pre = mm(S[...], Wi[cols, :], NT) + IB[:, cols]
        sig = jax.nn.sigmoid(pre)
        H[:, cols] = (pre * sig).astype(BF16)
        DV[:, cols] = sig * (1.0 + pre * (1.0 - sig))
        return 0

    mine, theirs = part(core, CORE), part(1 - core, CORE)

    one_hot_sel(core)
    l_series.wait()
    p_own[:1, :] = ob_ref[...].reshape(1, D)
    lax.fori_loop(0, 3, sel_body, 0)
    forward_first(0)
    make_perm(0)
    forward_first(1)
    make_perm(1)
    forward_first(2)
    make_perm(2)
    forward_first(3)
    forward_second(0)
    relay(0, 0)
    transposed(0, 0, sH)
    forward_first(4)
    forward_second(1)
    relay(1, 0)
    l_t.wait()
    lax.fori_loop(0, 2, spread_body, 0)
    forward_second(4)
    forward_second(2)
    relay(2, 0)
    lax.fori_loop(2, 4, spread_body, 0)
    forward_first(5)
    forward_second(3)
    relay(3, 0)
    forward_second(5)
    relay(0, 1)
    lax.fori_loop(4, 5, spread_body, 0)
    relay(4, 0)
    relay(1, 1)
    transposed(0, 1, sH)
    relay(2, 1)
    relay(5, 0)
    transposed(0, 2, sH)
    relay(3, 1)
    arrived(0)
    arrived(1)
    b_crossed.wait_recv()
    lax.fori_loop(0, 2, hidden_body, 0, unroll=True)
    relay(4, 1)
    lax.fori_loop(2, 3, hidden_body, 0)
    relay(5, 1)
    arrived(2)
    arrived(3)

    def skip_body(i, _):
        cols = part(i, 256)
        p_send[i] = mm(sH[theirs, :], Ws[:, cols])
        p_own[:, cols] = mm(sH[mine, :], Ws[:, cols])
        return 0

    lax.fori_loop(0, D // 256, skip_body, 0, unroll=True)
    arrived(4)
    arrived(5)

    p_copies = []
    for i in range(D // 256):
        cols = pl.ds(i * 256, 256)
        p_send[i] = p_send[i] + mm(H[theirs, :], Wo[:, cols])
        p_copies.append(send(p_send.at[i], p_recv.at[i], partner))

    def predict_body(i, _):
        cols = part(i, 256)
        p_own[:, cols] = p_own[:, cols] + mm(H[mine, :], Wo[:, cols])
        return 0

    lax.fori_loop(0, D // 256, predict_body, 0, unroll=True)
    for c in p_copies:
        c.wait_recv()

    def slope_body(w, _):
        rows = part(w, PATCHES)
        count = counts_ref[(x_hi * 2 + core) * (CORE // PATCHES) + w]
        counted = jnp.full((PATCHES, 128), count, jnp.int32)
        valid = lax.broadcasted_iota(jnp.int32, (PATCHES, 128), 0) < counted
        weight = (jnp.where(valid, 1.0, 0.0) / counted.astype(F32))[:, :1]
        for i in range(D // 256):
            cols = pl.ds(i * 256, 256)
            residue = spread[rows, cols] - (p_own[rows, cols] + p_recv[i, rows, :])
            t = tau[:, cols]
            slopes = jnp.where(residue >= 0, t, 1.0 - t) * jnp.clip(
                residue / HUBER_WIDTH, -1.0, 1.0
            )
            OG[pl.ds(pl.multiple_of(core * CORE + w * PATCHES, PATCHES), PATCHES), cols] = (
                -slopes * weight
            ).astype(BF16)
        return 0

    og_copies = []
    for i in range(2):
        lax.fori_loop(8 * i, 8 * i + 8, slope_body, 0)
        rows = OG.at[part(core * 2 + i, 128), :]
        og_copies.append(send(rows, rows, partner))

    def backflow(rows):
        def body(i, _):
            cols = part(i, 256)
            back = mm(OG[rows, :], Wo[cols, :], NT)
            HG[rows, cols] = (back * DV[rows, cols]).astype(BF16)
            return 0

        lax.fori_loop(0, HALF // 256, body, 0, unroll=True)

    backflow(mine)
    for c in og_copies:
        c.wait_recv()

    def lanes(g, h):
        return pl.ds(GROUPS[g][1] + h * GROUPS[g][2], GROUPS[g][2])

    def half_lanes(g):
        return pl.ds(GROUPS[g][1] // 2, GROUPS[g][2])

    def ring_start(axis, g, view, ra, rd):
        p = pos[axis]
        up, down = along(axis, 1), along(axis, 3)
        to = half_lanes(g)
        return (
            send(view(rem(p + 2, 4), lanes(g, 0)), ra.at[0, :, to], up),
            send(view(rem(p + 2, 4), lanes(g, 1)), ra.at[1, :, to], down),
            send(view(rem(p + 1, 4), lanes(g, 1)), rd.at[0, :, to], up),
            send(view(rem(p + 3, 4), lanes(g, 0)), rd.at[1, :, to], down),
        )

    def ring_pass(axis, g, size, rows, base, ra, out, rsum, own, step):
        p = pos[axis]
        to = half_lanes(g)
        passed = []
        for h, hop in ((0, 1), (1, 3)):
            step[h].wait_recv()

            def body(i, _, h=h, hop=hop):
                there = pl.ds(
                    pl.multiple_of(base + rem(p + hop, 4) * size + i * rows, 8), rows
                )
                here = part(i, rows)
                out[h, here, to] = (
                    own[there, lanes(g, h)] + ra[h, here, to].astype(F32)
                ).astype(BF16)
                return 0

            lax.fori_loop(0, size // rows, body, 0)
            passed.append(send(out.at[h, :, to], rsum.at[h, :, to], along(axis, hop)))
        return passed

    def ring_end(axis, g, size, rows, base, rsum, rd, own, dst, step, passed):
        p = pos[axis]
        to = half_lanes(g)
        for c in (step[2], step[3], passed[0], passed[1]):
            c.wait_recv()

        def body(i, _):
            there = pl.ds(pl.multiple_of(base + p * size + i * rows, 8), rows)
            here = part(i, rows)
            for h in range(2):
                dst[here, lanes(g, h)] = (
                    own[there, lanes(g, h)]
                    + rsum[h, here, to].astype(F32)
                    + rd[1 - h, here, to].astype(F32)
                )
            return 0

        lax.fori_loop(0, size // rows, body, 0)

    steps = {}

    def gradient(k, right):
        for g, (order, start, width) in enumerate(GROUPS):
            def body(i, _, g=g):
                cols = part(i, 256)
                value = mm(LT[k, g], right[:, cols])
                G[k, :, cols] = value
                ST[k, :, cols] = value.astype(BF16)
                return 0

            lax.fori_loop(start // 256, (start + 2 * width) // 256, body, 0, unroll=True)
            steps[k, g, 0] = ring_start(
                order[0], g, lambda q, cols: ST.at[k, part(q, C1), cols], RA.at[k], RD.at[k]
            )

    def pass_on(k):
        for g, (order, _, _) in enumerate(GROUPS):
            steps[k, g, 1] = ring_pass(
                order[0], g, C1, 32, 0, RA.at[k], T2.at[k], RSUM.at[k], G.at[k], steps[k, g, 0]
            )

    def second_phase(k):
        for g, (order, start, width) in enumerate(GROUPS):
            ring_end(
                order[0], g, C1, 32, 0, RSUM.at[k], RD.at[k], G.at[k], acc1.at[k],
                steps[k, g, 0], steps[k, g, 1],
            )
            cols = pl.ds(start, 2 * width)
            for q in range(4):
                ST2[k, q, :, cols] = acc1[k, pl.ds(q * C2, C2), cols].astype(BF16)
            steps[k, g, 2] = ring_start(
                order[1], g, lambda q, cols: ST2.at[k, q, :, cols], RA2.at[k], RD2.at[k]
            )

    def pass_on_second(k):
        for g, (order, _, _) in enumerate(GROUPS):
            steps[k, g, 3] = ring_pass(
                order[1], g, C2, C2, 0, RA2.at[k], T3.at[k], RSUM2.at[k], acc1.at[k],
                steps[k, g, 2],
            )

    def third_phase(k):
        for g, (order, start, width) in enumerate(GROUPS):
            ring_end(
                order[1], g, C2, C2, 0, RSUM2.at[k], RD2.at[k], acc1.at[k], acc2.at[k],
                steps[k, g, 2], steps[k, g, 3],
            )
            cols = pl.ds(start, 2 * width)
            for q in range(4):
                piece = acc2[k, pl.ds(q * C3, C3), cols]
                F3[k, q, :, cols] = piece
                ST3[k, q, :, cols] = piece.astype(BF16)
            p3 = pos[order[2]]
            steps[k, g, 4] = [
                send(
                    ST3.at[k, rem(p3 + o, 4), :, cols], R3.at[k, o - 1, :, cols],
                    along(order[2], o),
                )
                for o in (1, 3, 2)
            ]

    rescale = 1.0 / 2048

    def finish(k, out):
        for g, (order, start, width) in enumerate(GROUPS):
            for c in steps[k, g, 4]:
                c.wait_recv()
            cols = pl.ds(start, 2 * width)
            total = F3[k, pos[order[2]], :, cols]
            for o in range(3):
                total = total + R3[k, o, :, cols].astype(F32)
            out[:, cols] = total * rescale

    gradient(0, OG)
    for g in range(3):
        transposed(1, g, H)
    gradient(1, OG)
    backflow(theirs)
    for g in range(3):
        transposed(2, g, HG)
    pass_on(0)
    gradient(2, S)
    pass_on(1)

    bsend[0, :, pl.ds(0, HALF)] = jnp.sum(HG[...].astype(F32), axis=0, keepdims=True)
    bsend[0, :, pl.ds(HALF, D)] = jnp.sum(OG[...].astype(F32), axis=0, keepdims=True)

    def bias_send(i):
        axis = "xyz"[i]
        return [send(bsend.at[i], brecv.at[i, o - 1], along(axis, o)) for o in (1, 2, 3)]

    def bias_add(i, copies):
        for c in copies:
            c.wait_recv()
        bsend[i + 1] = bsend[i] + brecv[i, 0] + brecv[i, 1] + brecv[i, 2]

    bias1 = bias_send(0)
    for i in range(CHIP // 256):
        rows = pl.ds(i * 256, 256)
        igp[:, rows] = mm(Wi[...], HG[rows, :], TT)
    igp_copies = []
    for j in range(2):
        rows = pl.ds(pl.multiple_of(j * 640 + (1 - core) * SHARD, 64), SHARD)
        igp_copies.append(send(igp.at[rows, :], igp_recv.at[j], partner))
    second_phase(0)
    pass_on(2)
    for i in range(CHIP // 256):
        rows = pl.ds(i * 256, 256)
        igf[:, rows] = mm(Ws[...], OG[rows, :], NT)
    for c in igp_copies:
        c.wait_recv()

    def columns(hi):
        here = pl.ds(pl.multiple_of(hi * PAD, 128), SHARD)
        there = pl.ds(pl.multiple_of(hi * 640 + core * SHARD, 64), SHARD)
        return igf[here, :] + igp[there, :] + igp_recv[hi]

    ig_send[...] = columns(other_hi).astype(BF16)
    igf[own_rows, :] = columns(x_hi)
    lower, upper = pl.ds(0, SHARD // 2), pl.ds(SHARD // 2, SHARD // 2)
    ig1 = (
        send(ig_send.at[lower, :], ig_mid.at[lower, :], along("x", 1)),
        send(ig_send.at[upper, :], ig_mid.at[upper, :], along("x", 3)),
    )
    out0 = pltpu.make_async_copy(
        igf.at[own_rows, :], in_out.at[:, part(x_hi, CHIP)], lsem.at[len(loads)]
    )
    out0.start()
    second_phase(1)
    bias_add(0, bias1)
    bias2 = bias_send(1)
    pass_on_second(0)
    second_phase(2)
    pass_on_second(1)
    third_phase(0)
    for c in ig1:
        c.wait_recv()
    ig2 = (
        send(ig_mid.at[lower, :], ig_recv.at[lower, :], along("x", 1)),
        send(ig_mid.at[upper, :], ig_recv.at[upper, :], along("x", 3)),
    )
    pass_on_second(2)
    bias_add(1, bias2)
    bias3 = bias_send(2)
    third_phase(1)
    third_phase(2)
    for c in ig2:
        c.wait_recv()
    others = pl.ds(pl.multiple_of(other_hi * PAD, 128), SHARD)
    igf[others, :] = ig_recv[...].astype(F32)
    out1 = pltpu.make_async_copy(
        igf.at[others, :], in_out.at[:, part(other_hi, CHIP)], lsem.at[len(loads) + 1]
    )
    out1.start()
    bias_add(2, bias3)

    def pick(v, start):
        n = v.shape[1]
        i = lax.broadcasted_iota(jnp.int32, (n, 128), 0)
        j = lax.broadcasted_iota(jnp.int32, (n, 128), 1)
        hot = jnp.where(i == j + start, 1.0, 0.0).astype(F32)
        return lax.dot_general(
            jnp.broadcast_to(v, (8, n)), hot, NN,
            precision=lax.Precision.HIGHEST, preferred_element_type=F32,
        )[:1] * rescale

    ib_out[...] = pick(bsend[3, :, pl.ds(0, HALF)], x_hi * PAD + dp * 10)[:, :10]
    ob_out[...] = pick(bsend[3, :, pl.ds(HALF, D)], dp * 40)[:, :40]
    finish(0, gs_out)
    finish(1, go_out)
    finish(2, gi_out)
    assert len(sent) == N_SENDS
    for c in sent:
        c.wait_send()
    out0.wait()
    out1.wait()


N_SENDS = 218


def write_out(*refs):
    ins, outs, (big, grads, b10, b40, sem_in, sem_out) = refs[:6], refs[6:12], refs[12:]
    hops = [
        (ins[0].at[part(i, 80), :], big.at[part(i, 80), :], outs[0].at[part(i, 80), :])
        for i in range(4)
    ]
    hops += [(ins[i], grads.at[i - 1], outs[i]) for i in (1, 2, 3)]
    hops += [(ins[4], b10, outs[4]), (ins[5], b40, outs[5])]
    copies = []
    for i, (src, mid, dst) in enumerate(hops):
        c = pltpu.make_async_copy(src, mid, sem_in.at[i])
        c.start()
        copies.append((c, pltpu.make_async_copy(mid, dst, sem_out.at[i])))
    for a, b in copies:
        a.wait()
        b.start()
    for _, b in copies:
        b.wait()


def on_device(series, wi, ib, wo, ws, ob, targets, levels, counts):
    hbm = pl.BlockSpec(memory_space=pl.ANY)
    vmem = pl.BlockSpec(memory_space=pltpu.VMEM)
    smem = pl.BlockSpec(memory_space=pltpu.SMEM)
    grad = jax.ShapeDtypeStruct((C3, D), F32)
    shapes = (
        jax.ShapeDtypeStruct((SHARD, 2 * CHIP), F32), grad, grad, grad,
        jax.ShapeDtypeStruct((1, 10), F32), jax.ShapeDtypeStruct((1, 40), F32),
    )
    results = pl.pallas_call(
        kernel,
        out_shape=shapes,
        in_specs=[hbm] * 4 + [vmem] * 2 + [hbm] + [smem] * 2,
        out_specs=(hbm,) + (vmem,) * 5,
        scratch_shapes=[
            pltpu.VMEM((CHIP, D), BF16),
            pltpu.VMEM((HALF, D), BF16),
            pltpu.VMEM((HALF, D), BF16),
            pltpu.VMEM((HALF, D), BF16),
            pltpu.VMEM((1, HALF), F32),
            pltpu.VMEM((CORE, 128), F32),
            pltpu.VMEM((HALF, D), BF16),
            pltpu.VMEM((3, OWN, HALF), BF16),
            pltpu.VMEM((CHIP, HALF), BF16),
            pltpu.VMEM((CHIP, HALF), BF16),
            pltpu.VMEM((CHIP, HALF), F32),
            pltpu.VMEM((3, 3, OWN, CHIP), BF16),
            pltpu.VMEM((CHIP, HALF), BF16),
            pltpu.VMEM((CHIP, D), BF16),
            pltpu.VMEM((CORE, D), F32),
            pltpu.VMEM((1, D), F32),
            pltpu.VMEM((5, CORE, 256), F32),
            pltpu.VMEM((5, CORE, 256), F32),
            pltpu.VMEM((CORE, D), F32),
            pltpu.VMEM((3, OWN, D), F32),
            pltpu.VMEM((3, OWN, D), BF16),
            pltpu.VMEM((3, 2, C1, LANES), BF16),
            pltpu.VMEM((3, 2, C1, LANES), BF16),
            pltpu.VMEM((3, 2, C1, LANES), BF16),
            pltpu.VMEM((3, 2, C1, LANES), BF16),
            pltpu.VMEM((3, C1, D), F32),
            pltpu.VMEM((3, 4, C2, D), BF16),
            pltpu.VMEM((3, 2, C2, LANES), BF16),
            pltpu.VMEM((3, 2, C2, LANES), BF16),
            pltpu.VMEM((3, 2, C2, LANES), BF16),
            pltpu.VMEM((3, 2, C2, LANES), BF16),
            pltpu.VMEM((3, C2, D), F32),
            pltpu.VMEM((3, 4, C3, D), F32),
            pltpu.VMEM((3, 4, C3, D), BF16),
            pltpu.VMEM((3, 3, C3, D), BF16),
            pltpu.VMEM((4, 1, HALF + D), F32),
            pltpu.VMEM((3, 3, 1, HALF + D), F32),
            pltpu.VMEM((D, CHIP), F32),
            pltpu.VMEM((2, SHARD, CHIP), F32),
            pltpu.VMEM((HALF, CHIP), F32),
            pltpu.VMEM((SHARD, CHIP), BF16),
            pltpu.VMEM((SHARD, CHIP), BF16),
            pltpu.VMEM((SHARD, CHIP), BF16),
            pltpu.SemaphoreType.DMA((8,)),
            pltpu.SemaphoreType.DMA((N_SENDS,)),
            pltpu.SemaphoreType.DMA((N_SENDS,)),
        ],
        compiler_params=pltpu.CompilerParams(
            collective_id=0, has_side_effects=True, vmem_limit_bytes=63 * 1024 * 1024
        ),
    )(series, wi, wo, ws, ib, ob, targets, levels, counts)
    input_grad, inner, outer, skip, inbias, outbias = pl.pallas_call(
        write_out,
        out_shape=shapes,
        in_specs=[hbm] * 6,
        out_specs=(hbm,) * 6,
        scratch_shapes=[
            pltpu.VMEM((SHARD, 2 * CHIP), F32),
            pltpu.VMEM((3, C3, D), F32),
            pltpu.VMEM((1, 10), F32),
            pltpu.VMEM((1, 40), F32),
            pltpu.SemaphoreType.DMA((9,)),
            pltpu.SemaphoreType.DMA((9,)),
        ],
    )(*results)
    return input_grad.T, inner, outer, skip, inbias.reshape(10), outbias.reshape(40)


def solution(mesh):
    return jax.shard_map(
        on_device,
        mesh=mesh,
        in_specs=(
            P("dp", None), P("mp", None), P("mp"), P("mp", None), P("mp", None), P(None),
            P("dp", None), P(None), P("dp"),
        ),
        out_specs=(
            P("dp", "mp"), P(("mp", "dp"), None), P(("mp", "dp"), None), P(("mp", "dp"), None),
            P(("mp", "dp")), P("dp"),
        ),
        check_vma=False,
    )
```

```python
import jax
import jax.numpy as jnp
from jax import lax
from jax.experimental import pallas as pl
from jax.experimental.pallas import tpu as pltpu
from jax.sharding import PartitionSpec as P

MESH = pl.DeviceIdType.MESH
F32 = jnp.float32
BF16 = jnp.bfloat16
LEVELS = 9
PATCHES = 16
QUANTILES = 10
HUBER_WIDTH = 0.5

D = 1280
SHARD = 320
PAD = 384
HALF = 2 * PAD
CHIP = 512
CORE = 256
OWN = 640
C1, C2, C3 = 160, 40, 10
LANES = 640

NN = (((1,), (0,)), ((), ()))
NT = (((1,), (1,)), ((), ()))
TT = (((0,), (1,)), ((), ()))


def mm(a, b, dims=NN):
    return lax.dot_general(a, b, dims, preferred_element_type=F32)


def rem(a, n):
    return lax.rem(a, jnp.int32(n))


def div(a, n):
    return lax.div(a, jnp.int32(n))


def part(index, size):
    return pl.ds(pl.multiple_of(index * size, size), size)


GROUPS = (("yxz", 0, 256), ("zyx", 512, 256), ("xzy", 1024, 128))


def split(n, size):
    q = (
        (n >= size).astype(jnp.int32)
        + (n >= 2 * size).astype(jnp.int32)
        + (n >= 3 * size).astype(jnp.int32)
    )
    return q, n - q * size


def natural(n, order):
    d1, n = split(n, C1)
    d2, n = split(n, C2)
    d3, r = split(n, C3)
    at = dict(zip(order, (d1, d2, d3)))
    x_hi = (at["x"] >= 2).astype(jnp.int32)
    x_lo = at["x"] - 2 * x_hi
    return x_hi * PAD + (at["z"] * 8 + x_lo * 4 + at["y"]) * 10 + r


def kernel(
    series_hbm, wi_hbm, wo_hbm, ws_hbm, ib_ref, ob_ref, targets_hbm, levels_ref, counts_ref,
    in_out, gi_out, go_out, gs_out, ib_out, ob_out,
    S, Wi, Wo, Ws, IB, T, sel, perm, sH, H, DV, LT, HG, OG,
    spread, tau, p_send, p_recv, p_own, G, ST, RA, RD, RSUM, T2,
    acc1, ST2, RA2, RD2, RSUM2, T3, acc2, F3, ST3, R3,
    bsend, brecv, igp, igp_recv, igf, ig_send, ig_mid, ig_recv,
    lsem, ssem, rsem,
):
    dp = lax.axis_index("dp")
    mp = lax.axis_index("mp")
    core = rem(mp, 2)
    x_hi = div(mp, 2)
    z = div(dp, 8)
    x_lo = rem(div(dp, 4), 2)
    y = rem(dp, 4)
    x = x_hi * 2 + x_lo
    other_hi = 1 - x_hi

    def device(x, y, z, core):
        return {"dp": z * 8 + rem(x, 2) * 4 + y, "mp": div(x, 2) * 2 + core}

    pos = {"x": x, "y": y, "z": z}

    def along(axis, k):
        at = dict(pos)
        at[axis] = rem(at[axis] + k, 4)
        return device(at["x"], at["y"], at["z"], core)

    partner = device(x, y, z, 1 - core)
    cross = device(3 - x, y, z, core)
    beside = device(x + 1 - 2 * x_lo, y, z, core)

    loads = []

    def load(src, dst):
        c = pltpu.make_async_copy(src, dst, lsem.at[len(loads)])
        c.start()
        loads.append(c)
        return c

    own_rows = pl.ds(pl.multiple_of(x_hi * PAD, 128), SHARD)
    l_i = load(wi_hbm, Wi.at[own_rows, :])
    l_s = load(ws_hbm, Ws.at[own_rows, :])
    l_o = load(wo_hbm, Wo.at[own_rows, :])
    l_series = load(series_hbm.at[part(x_hi, CHIP), :], S)
    l_t = load(targets_hbm.at[part(x_hi * 2 + core, CORE), :], T)

    IB[:, part(x_hi, PAD)] = jnp.concatenate(
        [ib_ref[...].reshape(1, SHARD), jnp.zeros((1, PAD - SHARD), F32)], axis=1
    )
    barrier = pltpu.get_barrier_semaphore()
    peers = [partner] + [along(a, k) for a in "xyz" for k in (1, 2, 3)]
    for peer in peers:
        pl.semaphore_signal(barrier, inc=1, device_id=peer, device_id_type=MESH)
    pl.semaphore_wait(barrier, len(peers))

    sent = []

    def send(src, dst, to):
        i = len(sent)
        c = pltpu.make_async_remote_copy(
            src_ref=src, dst_ref=dst, send_sem=ssem.at[i], recv_sem=rsem.at[i],
            device_id=to, device_id_type=MESH,
        )
        c.start()
        sent.append(c)
        return c

    weights = (Wi, Ws, Wo)
    axis_of = (y, z)

    def quarter(w, hi, color, q, start, size):
        return weights[w].at[
            pl.ds(pl.multiple_of(hi * PAD + q * 80, 16), 80),
            pl.ds(pl.multiple_of(color * LANES + start, 128), size),
        ]

    def on_color(color, a, b):
        return jnp.where(color == 0, a, b)

    first, second = x_lo, 1 - x_lo

    def ring(color):
        up = {k: on_color(color, along("y", 1)[k], along("z", 1)[k]) for k in ("dp", "mp")}
        down = {k: on_color(color, along("y", 3)[k], along("z", 3)[k]) for k in ("dp", "mp")}
        return on_color(color, y, z), up, down

    items = [
        (w, start, size, cut)
        for w in range(3)
        for start, size, cut in ((0, 384, 256 - 128 * (w % 2)), (384, 256, 128))
    ]
    crossed, beside_of, own_of, relayed = [], {}, {}, {}
    for i, (w, start, size, _) in enumerate(items):
        if i % 2 == 0:
            (l_i, l_s, l_o)[w].wait()
        piece = quarter(w, x_hi, second, on_color(second, y, z), start, size)
        crossed.append(send(piece, piece, cross))
        if w == 2:
            piece = quarter(w, x_hi, first, on_color(first, y, z), start, size)
            beside_of[i] = send(piece, piece, cross)
        if i == 1:
            own_bias = IB.at[:, part(x_hi, PAD)]
            b_crossed = send(own_bias, own_bias, cross)

    for W in weights:
        for j in range(2):
            W[pl.ds(j * PAD + SHARD, PAD - SHARD), :] = jnp.zeros((PAD - SHARD, D), BF16)

    def one_hot_sel(k):
        def body(i, _):
            h = lax.broadcasted_iota(jnp.int32, (128, D), 0) + i * 128
            col = lax.broadcasted_iota(jnp.int32, (128, D), 1)
            hi = (h >= PAD).astype(jnp.int32)
            j = h - hi * PAD
            want = hi * 640 + k * SHARD + j
            sel[part(i, 128), :] = jnp.where((col == want) & (j < SHARD), 1.0, 0.0).astype(BF16)
            return 0

        lax.fori_loop(0, HALF // 128, body, 0)

    def forward_first(i):
        w, start, size, _ = items[i]
        q, up, down = ring(first)
        crossed[i].wait_recv()
        piece = quarter(w, other_hi, first, q, start, size)
        if w < 2:
            beside_of[i] = send(piece, piece, beside)
        own_of[i, 0] = send(piece, piece, up), send(piece, piece, down)

    def forward_second(i):
        w, start, size, _ = items[i]
        q, up, down = ring(second)
        beside_of[i].wait_recv()
        piece = quarter(w, other_hi, second, q, start, size)
        own_of[i, 1] = send(piece, piece, up), send(piece, piece, down)

    def relay(i, turn):
        w, start, size, cut = items[i]
        color = (first, second)[turn]
        q, up, down = ring(color)
        from_below, from_above = own_of[i, turn]
        from_below.wait_recv()
        a = quarter(w, other_hi, color, rem(q + 3, 4), start, cut)
        s1 = send(a, a, up)
        from_above.wait_recv()
        b = quarter(w, other_hi, color, rem(q + 1, 4), start + cut, size - cut)
        relayed[i, turn] = s1, send(b, b, down)

    def arrived(i):
        for turn in range(2):
            for c in relayed[i, turn]:
                c.wait_recv()

    def sel_body(i, _):
        sH[:, part(i, 256)] = mm(S[...], sel[part(i, 256), :], NT).astype(BF16)
        return 0

    def make_perm(k):
        def body(i, _):
            n = lax.broadcasted_iota(jnp.int32, (128, 128), 0) + i * 128
            want = natural(n, GROUPS[k][0])
            lane = lax.broadcasted_iota(jnp.int32, (128, 128), 1)
            for t in range(HALF // 128):
                perm[k, part(i, 128), pl.ds(t * 128, 128)] = jnp.where(
                    lane + t * 128 == want, 1.0, 0.0
                ).astype(BF16)
            return 0

        lax.fori_loop(0, OWN // 128, body, 0)

    def transposed(k, g, src):
        def body(i, _):
            LT[k, g, :, part(i, 256)] = mm(perm[g], src[part(i, 256), :], NT).astype(BF16)
            return 0

        lax.fori_loop(0, CHIP // 256, body, 0, unroll=True)

    def spread_body(i, _):
        cols = part(i, 256)
        col = lax.broadcasted_iota(jnp.int32, (128, 256), 1) + i * 256
        row = lax.broadcasted_iota(jnp.int32, (128, 256), 0)
        off = col - row * QUANTILES
        spreader = jnp.where((off >= 0) & (off < QUANTILES), 1.0, 0.0).astype(F32)
        spread[:, cols] = (
            lax.dot_general(
                T[...], spreader, NN, precision=lax.Precision.HIGHEST, preferred_element_type=F32
            )
            - p_own[:1, cols]
        )
        rows = jnp.zeros((128, 256), F32)
        for c in range(QUANTILES):
            level = jnp.full((128, 256), levels_ref[c], jnp.int32).astype(F32) + 1.0
            rows = rows + jnp.where(off == c, level / (LEVELS + 1), 0.0)
        tau[:, cols] = jnp.sum(rows, axis=0, keepdims=True)
        return 0

    def hidden_body(i, _):
        cols = part(i, 256)
        pre = mm(S[...], Wi[cols, :], NT) + IB[:, cols]
        sig = jax.nn.sigmoid(pre)
        H[:, cols] = (pre * sig).astype(BF16)
        DV[:, cols] = sig * (1.0 + pre * (1.0 - sig))
        return 0

    mine, theirs = part(core, CORE), part(1 - core, CORE)

    one_hot_sel(core)
    l_series.wait()
    p_own[:1, :] = ob_ref[...].reshape(1, D)
    lax.fori_loop(0, 3, sel_body, 0)
    forward_first(0)
    make_perm(0)
    forward_first(1)
    make_perm(1)
    forward_first(2)
    make_perm(2)
    forward_first(3)
    forward_second(0)
    relay(0, 0)
    transposed(0, 0, sH)
    forward_first(4)
    forward_second(1)
    relay(1, 0)
    l_t.wait()
    lax.fori_loop(0, 2, spread_body, 0)
    forward_second(4)
    forward_second(2)
    relay(2, 0)
    lax.fori_loop(2, 4, spread_body, 0)
    forward_first(5)
    forward_second(3)
    relay(3, 0)
    forward_second(5)
    relay(0, 1)
    lax.fori_loop(4, 5, spread_body, 0)
    relay(4, 0)
    relay(1, 1)
    transposed(0, 1, sH)
    relay(2, 1)
    relay(5, 0)
    transposed(0, 2, sH)
    relay(3, 1)
    arrived(0)
    arrived(1)
    b_crossed.wait_recv()
    lax.fori_loop(0, 2, hidden_body, 0, unroll=True)
    relay(4, 1)
    lax.fori_loop(2, 3, hidden_body, 0)
    relay(5, 1)
    arrived(2)
    arrived(3)

    def skip_body(i, _):
        cols = part(i, 256)
        p_send[i] = mm(sH[theirs, :], Ws[:, cols])
        p_own[:, cols] = mm(sH[mine, :], Ws[:, cols])
        return 0

    lax.fori_loop(0, D // 256, skip_body, 0, unroll=True)
    arrived(4)
    arrived(5)

    p_copies = []
    for i in range(D // 256):
        cols = pl.ds(i * 256, 256)
        p_send[i] = p_send[i] + mm(H[theirs, :], Wo[:, cols])
        p_copies.append(send(p_send.at[i], p_recv.at[i], partner))

    def predict_body(i, _):
        cols = part(i, 256)
        p_own[:, cols] = p_own[:, cols] + mm(H[mine, :], Wo[:, cols])
        return 0

    lax.fori_loop(0, D // 256, predict_body, 0, unroll=True)
    for c in p_copies:
        c.wait_recv()

    def slope_body(w, _):
        rows = part(w, PATCHES)
        count = counts_ref[(x_hi * 2 + core) * (CORE // PATCHES) + w]
        counted = jnp.full((PATCHES, 128), count, jnp.int32)
        valid = lax.broadcasted_iota(jnp.int32, (PATCHES, 128), 0) < counted
        weight = (jnp.where(valid, 1.0, 0.0) / counted.astype(F32))[:, :1]
        for i in range(D // 256):
            cols = pl.ds(i * 256, 256)
            residue = spread[rows, cols] - (p_own[rows, cols] + p_recv[i, rows, :])
            t = tau[:, cols]
            slopes = jnp.where(residue >= 0, t, 1.0 - t) * jnp.clip(
                residue / HUBER_WIDTH, -1.0, 1.0
            )
            OG[pl.ds(pl.multiple_of(core * CORE + w * PATCHES, PATCHES), PATCHES), cols] = (
                -slopes * weight
            ).astype(BF16)
        return 0

    og_copies = []
    for i in range(2):
        lax.fori_loop(8 * i, 8 * i + 8, slope_body, 0)
        rows = OG.at[part(core * 2 + i, 128), :]
        og_copies.append(send(rows, rows, partner))

    def backflow(rows):
        def body(i, _):
            cols = part(i, 256)
            back = mm(OG[rows, :], Wo[cols, :], NT)
            HG[rows, cols] = (back * DV[rows, cols]).astype(BF16)
            return 0

        lax.fori_loop(0, HALF // 256, body, 0, unroll=True)

    backflow(mine)
    for c in og_copies:
        c.wait_recv()

    def lanes(g, h):
        return pl.ds(GROUPS[g][1] + h * GROUPS[g][2], GROUPS[g][2])

    def half_lanes(g):
        return pl.ds(GROUPS[g][1] // 2, GROUPS[g][2])

    def ring_start(axis, g, view, ra, rd):
        p = pos[axis]
        up, down = along(axis, 1), along(axis, 3)
        to = half_lanes(g)
        return (
            send(view(rem(p + 2, 4), lanes(g, 0)), ra.at[0, :, to], up),
            send(view(rem(p + 2, 4), lanes(g, 1)), ra.at[1, :, to], down),
            send(view(rem(p + 1, 4), lanes(g, 1)), rd.at[0, :, to], up),
            send(view(rem(p + 3, 4), lanes(g, 0)), rd.at[1, :, to], down),
        )

    def ring_pass(axis, g, size, rows, base, ra, out, rsum, own, step):
        p = pos[axis]
        to = half_lanes(g)
        passed = []
        for h, hop in ((0, 1), (1, 3)):
            step[h].wait_recv()

            def body(i, _, h=h, hop=hop):
                there = pl.ds(
                    pl.multiple_of(base + rem(p + hop, 4) * size + i * rows, 8), rows
                )
                here = part(i, rows)
                out[h, here, to] = (
                    own[there, lanes(g, h)] + ra[h, here, to].astype(F32)
                ).astype(BF16)
                return 0

            lax.fori_loop(0, size // rows, body, 0)
            passed.append(send(out.at[h, :, to], rsum.at[h, :, to], along(axis, hop)))
        return passed

    def ring_end(axis, g, size, rows, base, rsum, rd, own, dst, step, passed):
        p = pos[axis]
        to = half_lanes(g)
        for c in (step[2], step[3], passed[0], passed[1]):
            c.wait_recv()

        def body(i, _):
            there = pl.ds(pl.multiple_of(base + p * size + i * rows, 8), rows)
            here = part(i, rows)
            for h in range(2):
                dst[here, lanes(g, h)] = (
                    own[there, lanes(g, h)]
                    + rsum[h, here, to].astype(F32)
                    + rd[1 - h, here, to].astype(F32)
                )
            return 0

        lax.fori_loop(0, size // rows, body, 0)

    steps = {}

    def gradient(k, right, left=None):
        for g, (order, start, width) in enumerate(GROUPS):
            if left is not None:
                transposed(k, g, left)

            def body(i, _, g=g):
                cols = part(i, 256)
                value = mm(LT[k, g], right[:, cols])
                G[k, :, cols] = value
                ST[k, :, cols] = value.astype(BF16)
                return 0

            lax.fori_loop(start // 256, (start + 2 * width) // 256, body, 0, unroll=True)
            steps[k, g, 0] = ring_start(
                order[0], g, lambda q, cols: ST.at[k, part(q, C1), cols], RA.at[k], RD.at[k]
            )

    def pass_on(k):
        for g, (order, _, _) in enumerate(GROUPS):
            steps[k, g, 1] = ring_pass(
                order[0], g, C1, 32, 0, RA.at[k], T2.at[k], RSUM.at[k], G.at[k], steps[k, g, 0]
            )

    def second_phase(k):
        for g, (order, start, width) in enumerate(GROUPS):
            ring_end(
                order[0], g, C1, 32, 0, RSUM.at[k], RD.at[k], G.at[k], acc1.at[k],
                steps[k, g, 0], steps[k, g, 1],
            )
            cols = pl.ds(start, 2 * width)
            for q in range(4):
                ST2[k, q, :, cols] = acc1[k, pl.ds(q * C2, C2), cols].astype(BF16)
            steps[k, g, 2] = ring_start(
                order[1], g, lambda q, cols: ST2.at[k, q, :, cols], RA2.at[k], RD2.at[k]
            )

    def pass_on_second(k):
        for g, (order, _, _) in enumerate(GROUPS):
            steps[k, g, 3] = ring_pass(
                order[1], g, C2, C2, 0, RA2.at[k], T3.at[k], RSUM2.at[k], acc1.at[k],
                steps[k, g, 2],
            )

    def third_phase(k):
        for g, (order, start, width) in enumerate(GROUPS):
            ring_end(
                order[1], g, C2, C2, 0, RSUM2.at[k], RD2.at[k], acc1.at[k], acc2.at[k],
                steps[k, g, 2], steps[k, g, 3],
            )
            cols = pl.ds(start, 2 * width)
            for q in range(4):
                piece = acc2[k, pl.ds(q * C3, C3), cols]
                F3[k, q, :, cols] = piece
                ST3[k, q, :, cols] = piece.astype(BF16)
            p3 = pos[order[2]]
            steps[k, g, 4] = [
                send(
                    ST3.at[k, rem(p3 + o, 4), :, cols], R3.at[k, o - 1, :, cols],
                    along(order[2], o),
                )
                for o in (2, 1, 3)
            ]

    rescale = 1.0 / 2048

    def finish(k, out):
        for g, (order, start, width) in enumerate(GROUPS):
            for c in steps[k, g, 4]:
                c.wait_recv()
            cols = pl.ds(start, 2 * width)
            total = F3[k, pos[order[2]], :, cols]
            for o in range(3):
                total = total + R3[k, o, :, cols].astype(F32)
            out[:, cols] = total * rescale

    gradient(0, OG)
    gradient(1, OG, H)
    backflow(theirs)
    for g in range(3):
        transposed(2, g, HG)
    pass_on(0)
    gradient(2, S)
    pass_on(1)

    bsend[0, :, pl.ds(0, HALF)] = jnp.sum(HG[...].astype(F32), axis=0, keepdims=True)
    bsend[0, :, pl.ds(HALF, D)] = jnp.sum(OG[...].astype(F32), axis=0, keepdims=True)

    def bias_send(i):
        axis = "xyz"[i]
        return [send(bsend.at[i], brecv.at[i, o - 1], along(axis, o)) for o in (1, 2, 3)]

    def bias_add(i, copies):
        for c in copies:
            c.wait_recv()
        bsend[i + 1] = bsend[i] + brecv[i, 0] + brecv[i, 1] + brecv[i, 2]

    bias1 = bias_send(0)
    for i in range(CHIP // 256):
        rows = pl.ds(i * 256, 256)
        igp[:, rows] = mm(Wi[...], HG[rows, :], TT)
    igp_copies = []
    for j in range(2):
        rows = pl.ds(pl.multiple_of(j * 640 + (1 - core) * SHARD, 64), SHARD)
        igp_copies.append(send(igp.at[rows, :], igp_recv.at[j], partner))
    second_phase(0)
    pass_on(2)
    for i in range(CHIP // 256):
        rows = pl.ds(i * 256, 256)
        igf[:, rows] = mm(Ws[...], OG[rows, :], NT)
    for c in igp_copies:
        c.wait_recv()

    def columns(hi):
        here = pl.ds(pl.multiple_of(hi * PAD, 128), SHARD)
        there = pl.ds(pl.multiple_of(hi * 640 + core * SHARD, 64), SHARD)
        return igf[here, :] + igp[there, :] + igp_recv[hi]

    ig_send[...] = columns(other_hi).astype(BF16)
    igf[own_rows, :] = columns(x_hi)
    lower, upper = pl.ds(0, SHARD // 2), pl.ds(SHARD // 2, SHARD // 2)
    ig1 = (
        send(ig_send.at[lower, :], ig_mid.at[lower, :], along("x", 1)),
        send(ig_send.at[upper, :], ig_mid.at[upper, :], along("x", 3)),
    )
    out0 = pltpu.make_async_copy(
        igf.at[own_rows, :], in_out.at[:, part(x_hi, CHIP)], lsem.at[len(loads)]
    )
    out0.start()
    second_phase(1)
    bias_add(0, bias1)
    bias2 = bias_send(1)
    pass_on_second(0)
    second_phase(2)
    pass_on_second(1)
    third_phase(0)
    for c in ig1:
        c.wait_recv()
    ig2 = (
        send(ig_mid.at[lower, :], ig_recv.at[lower, :], along("x", 1)),
        send(ig_mid.at[upper, :], ig_recv.at[upper, :], along("x", 3)),
    )
    pass_on_second(2)
    bias_add(1, bias2)
    bias3 = bias_send(2)
    third_phase(1)
    third_phase(2)
    for c in ig2:
        c.wait_recv()
    others = pl.ds(pl.multiple_of(other_hi * PAD, 128), SHARD)
    igf[others, :] = ig_recv[...].astype(F32)
    out1 = pltpu.make_async_copy(
        igf.at[others, :], in_out.at[:, part(other_hi, CHIP)], lsem.at[len(loads) + 1]
    )
    out1.start()
    bias_add(2, bias3)

    def pick(v, start):
        n = v.shape[1]
        i = lax.broadcasted_iota(jnp.int32, (n, 128), 0)
        j = lax.broadcasted_iota(jnp.int32, (n, 128), 1)
        hot = jnp.where(i == j + start, 1.0, 0.0).astype(F32)
        return lax.dot_general(
            jnp.broadcast_to(v, (8, n)), hot, NN,
            precision=lax.Precision.HIGHEST, preferred_element_type=F32,
        )[:1] * rescale

    ib_out[...] = pick(bsend[3, :, pl.ds(0, HALF)], x_hi * PAD + dp * 10)[:, :10]
    ob_out[...] = pick(bsend[3, :, pl.ds(HALF, D)], dp * 40)[:, :40]
    finish(0, gs_out)
    finish(1, go_out)
    finish(2, gi_out)
    assert len(sent) == N_SENDS
    for c in sent:
        c.wait_send()
    out0.wait()
    out1.wait()


N_SENDS = 218


def write_out(*refs):
    ins, outs, (big, grads, b10, b40, sem_in, sem_out) = refs[:6], refs[6:12], refs[12:]
    hops = [
        (ins[0].at[part(i, 80), :], big.at[part(i, 80), :], outs[0].at[part(i, 80), :])
        for i in range(4)
    ]
    hops += [(ins[i], grads.at[i - 1], outs[i]) for i in (1, 2, 3)]
    hops += [(ins[4], b10, outs[4]), (ins[5], b40, outs[5])]
    copies = []
    for i, (src, mid, dst) in enumerate(hops):
        c = pltpu.make_async_copy(src, mid, sem_in.at[i])
        c.start()
        copies.append((c, pltpu.make_async_copy(mid, dst, sem_out.at[i])))
    for a, b in copies:
        a.wait()
        b.start()
    for _, b in copies:
        b.wait()


def on_device(series, wi, ib, wo, ws, ob, targets, levels, counts):
    hbm = pl.BlockSpec(memory_space=pl.ANY)
    vmem = pl.BlockSpec(memory_space=pltpu.VMEM)
    smem = pl.BlockSpec(memory_space=pltpu.SMEM)
    grad = jax.ShapeDtypeStruct((C3, D), F32)
    shapes = (
        jax.ShapeDtypeStruct((SHARD, 2 * CHIP), F32), grad, grad, grad,
        jax.ShapeDtypeStruct((1, 10), F32), jax.ShapeDtypeStruct((1, 40), F32),
    )
    results = pl.pallas_call(
        kernel,
        out_shape=shapes,
        in_specs=[hbm] * 4 + [vmem] * 2 + [hbm] + [smem] * 2,
        out_specs=(hbm,) + (vmem,) * 5,
        scratch_shapes=[
            pltpu.VMEM((CHIP, D), BF16),
            pltpu.VMEM((HALF, D), BF16),
            pltpu.VMEM((HALF, D), BF16),
            pltpu.VMEM((HALF, D), BF16),
            pltpu.VMEM((1, HALF), F32),
            pltpu.VMEM((CORE, 128), F32),
            pltpu.VMEM((HALF, D), BF16),
            pltpu.VMEM((3, OWN, HALF), BF16),
            pltpu.VMEM((CHIP, HALF), BF16),
            pltpu.VMEM((CHIP, HALF), BF16),
            pltpu.VMEM((CHIP, HALF), F32),
            pltpu.VMEM((3, 3, OWN, CHIP), BF16),
            pltpu.VMEM((CHIP, HALF), BF16),
            pltpu.VMEM((CHIP, D), BF16),
            pltpu.VMEM((CORE, D), F32),
            pltpu.VMEM((1, D), F32),
            pltpu.VMEM((5, CORE, 256), F32),
            pltpu.VMEM((5, CORE, 256), F32),
            pltpu.VMEM((CORE, D), F32),
            pltpu.VMEM((3, OWN, D), F32),
            pltpu.VMEM((3, OWN, D), BF16),
            pltpu.VMEM((3, 2, C1, LANES), BF16),
            pltpu.VMEM((3, 2, C1, LANES), BF16),
            pltpu.VMEM((3, 2, C1, LANES), BF16),
            pltpu.VMEM((3, 2, C1, LANES), BF16),
            pltpu.VMEM((3, C1, D), F32),
            pltpu.VMEM((3, 4, C2, D), BF16),
            pltpu.VMEM((3, 2, C2, LANES), BF16),
            pltpu.VMEM((3, 2, C2, LANES), BF16),
            pltpu.VMEM((3, 2, C2, LANES), BF16),
            pltpu.VMEM((3, 2, C2, LANES), BF16),
            pltpu.VMEM((3, C2, D), F32),
            pltpu.VMEM((3, 4, C3, D), F32),
            pltpu.VMEM((3, 4, C3, D), BF16),
            pltpu.VMEM((3, 3, C3, D), BF16),
            pltpu.VMEM((4, 1, HALF + D), F32),
            pltpu.VMEM((3, 3, 1, HALF + D), F32),
            pltpu.VMEM((D, CHIP), F32),
            pltpu.VMEM((2, SHARD, CHIP), F32),
            pltpu.VMEM((HALF, CHIP), F32),
            pltpu.VMEM((SHARD, CHIP), BF16),
            pltpu.VMEM((SHARD, CHIP), BF16),
            pltpu.VMEM((SHARD, CHIP), BF16),
            pltpu.SemaphoreType.DMA((8,)),
            pltpu.SemaphoreType.DMA((N_SENDS,)),
            pltpu.SemaphoreType.DMA((N_SENDS,)),
        ],
        compiler_params=pltpu.CompilerParams(
            collective_id=0, has_side_effects=True, vmem_limit_bytes=63 * 1024 * 1024
        ),
    )(series, wi, wo, ws, ib, ob, targets, levels, counts)
    input_grad, inner, outer, skip, inbias, outbias = pl.pallas_call(
        write_out,
        out_shape=shapes,
        in_specs=[hbm] * 6,
        out_specs=(hbm,) * 6,
        scratch_shapes=[
            pltpu.VMEM((SHARD, 2 * CHIP), F32),
            pltpu.VMEM((3, C3, D), F32),
            pltpu.VMEM((1, 10), F32),
            pltpu.VMEM((1, 40), F32),
            pltpu.SemaphoreType.DMA((9,)),
            pltpu.SemaphoreType.DMA((9,)),
        ],
    )(*results)
    return input_grad.T, inner, outer, skip, inbias.reshape(10), outbias.reshape(40)


def solution(mesh):
    return jax.shard_map(
        on_device,
        mesh=mesh,
        in_specs=(
            P("dp", None), P("mp", None), P("mp"), P("mp", None), P("mp", None), P(None),
            P("dp", None), P(None), P("dp"),
        ),
        out_specs=(
            P("dp", "mp"), P(("mp", "dp"), None), P(("mp", "dp"), None), P(("mp", "dp"), None),
            P(("mp", "dp")), P("dp"),
        ),
        check_vma=False,
    )
```
